32 devices in a mesh: fsdp: 8 (over z, y), dom: 4 (over x, core).
Axes of the slice: x: 2, y: 2, z: 4, core: 2. Of those that a mesh axis runs over, the one named last changes fastest.
Arguments:
- hidden_states: bfloat16 [256, 128, 768], P(('fsdp', 'dom')), may hold values from -40 to 40
- title_tokens: int32 [256, 128], P(('fsdp', 'dom')), may hold values from 0 to 30521, as said below
- query_key_value: bfloat16 [768, 2304], P('fsdp'), may hold values from -0.5 to 2.5
- output_weight: bfloat16 [768, 768], P('fsdp'), may hold values from -0.21875 to 0.21875
- up_weight: bfloat16 [768, 3072], P('fsdp'), may hold values from -0.21875 to 0.21875
- down_weight: bfloat16 [3072, 768], P('fsdp'), may hold values from -0.109375 to 0.109375
- attention_gain: float32 [768], replicated, may hold values from 0.25 to 1.75
- feedforward_gain: float32 [768], replicated, may hold values from 0.25 to 1.75
- encoded: bfloat16 [16384, 768], P(('fsdp', 'dom')), may hold values from -6 to 6
- send_rows: int32 [32, 32, 48], P(('fsdp', 'dom')), may hold values from 0 to 511
- send_count: int32 [32, 32], P(('fsdp', 'dom')), may hold values from 6 to 48, as said below
- arrival_nodes: int32 [32, 32, 48], P(('fsdp', 'dom')), may hold values from 0 to 511
- sage_weight: bfloat16 [2, 768, 1024], P(None, 'fsdp'), may hold values from -0.21875 to 0.21875
- node_gain: float32 [1024], replicated, may hold values from 0.25 to 1.75
Outputs:
- title_vectors: bfloat16 [256, 768], P(('fsdp', 'dom'))
- node_output: bfloat16 [16384, 1024], P(('fsdp', 'dom'))
The draws below stay inside these ranges and needn't reach their ends.
Inputs may be any that keep to these rules, and one draw needn't show every extreme that they name: `title_tokens`: in each title the nonzero ids come first and zeros fill the rest; at least 16 ids of every title are nonzero. `send_count`: in every draw some device receives exactly 48 valid slots from every device.
All inputs are finite; a program needn't handle non-finite values.
Results may differ from the reference program's by a relative error of at most 0.0056.
Values may be sent and summed in bfloat16 or wider, within the bound.
A program may use at most 192 MiB of HBM per device.

```python
import math
import jax
import jax.numpy as jnp
from jax import lax

D = 768
HEADS = 12
HEAD_DIM = 64
FF = 3072
VOCAB = 30522
H = 1024
SEQ = 128
CAP = 48
TITLES_DEV = 8
NODES_DEV = 512
TITLES = 256
NODES = 16384
DEVICES = 32


def draw_hidden_states(key, part):
    streams = jax.random.split(key, 3)
    shape = (TITLES, SEQ, D)
    column_scale = jnp.exp(jax.random.uniform(streams[1], (D,), jnp.float32, math.log(0.3), math.log(3.0)))
    base = jax.random.normal(streams[0], shape, jnp.float32)
    row_scale = jnp.exp(jax.random.uniform(streams[2], (TITLES, SEQ, 1), jnp.float32, math.log(0.5), math.log(2.0)))
    values = base * row_scale * column_scale
    return jnp.clip(values, -40.0, 40.0).astype(jnp.bfloat16)


def draw_title_tokens(key, part):
    streams = jax.random.split(key, 2)
    lengths = jax.random.randint(streams[0], (TITLES, 1), SEQ // 8, SEQ + 1)
    idents = jax.random.randint(streams[1], (TITLES, SEQ), 1, VOCAB)
    position = jnp.arange(SEQ)[None, :]
    return jnp.where(position < lengths, idents, 0).astype(jnp.int32)


def draw_query_key_value(key, part):
    values = jnp.clip(jax.random.normal(key, (D, 3 * D), jnp.float32) * (1.0 / math.sqrt(D)), -0.5, 0.5)
    return values.astype(jnp.bfloat16)


def draw_send_count(key, part):
    streams = jax.random.split(key, 2)
    base = jax.random.randint(streams[0], (DEVICES, DEVICES), CAP // 8, CAP // 2 + 1)
    hottest = jax.random.randint(streams[1], (), 0, DEVICES)
    columns = jnp.arange(DEVICES)
    return jnp.where(columns[None, :] == hottest, CAP, base).astype(jnp.int32)


def draw_arrival_nodes(key, part):
    streams = jax.random.split(key, 3)
    shape = (DEVICES, DEVICES, CAP)
    first = jax.random.randint(streams[0], shape, 0, NODES_DEV)
    second = jax.random.randint(streams[1], shape, 0, NODES_DEV)
    lower = jnp.minimum(first, second).reshape(DEVICES, DEVICES * CAP)
    orders = jax.vmap(lambda stream: jax.random.permutation(stream, NODES_DEV))(jax.random.split(streams[2], DEVICES))
    picked = jnp.take_along_axis(orders.astype(jnp.int32), lower.astype(jnp.int32), axis=1)
    return picked.reshape(shape).astype(jnp.int32)


def place_ends(entries, own_key, least, top_value):
    index_at = [jax.random.randint(jax.random.fold_in(own_key, axis), (), 0, length) for axis, length in enumerate(entries.shape)]
    main_axis = entries.shape.index(max(entries.shape))
    beside = index_at[:main_axis] + [(index_at[main_axis] + 1) % entries.shape[main_axis]] + index_at[main_axis + 1:]
    return entries.at[tuple(index_at)].set(least).at[tuple(beside)].set(top_value)


def block_levels(rng, dims, pieces, least, largest):
    level = 1.0
    for axis_at, parts in pieces:
        heights = jax.random.uniform(jax.random.fold_in(jax.random.fold_in(rng, 6), axis_at), (parts,), jnp.float32, least / len(pieces), largest / len(pieces))
        level = level * jnp.repeat(jnp.exp(heights), dims[axis_at] // parts).reshape((-1,) + (1,) * (len(dims) - 1 - axis_at))
    return level


def gaussian(own_key, dims, scale, most, cuts=(), kind=jnp.bfloat16):
    level = block_levels(own_key, dims, cuts, -0.22, 0.18) if cuts else 1.0
    entries = jax.random.normal(own_key, dims, jnp.float32) * scale * level
    return jnp.minimum(jnp.maximum(entries, -most), most).astype(kind)


def setup_inputs(seed: int = 0) -> dict:
    key_of = jax.random.split(jax.random.key(seed), 15)
    hidden_states = draw_hidden_states(jax.random.fold_in(key_of[14], 71), 0)
    title_tokens = draw_title_tokens(jax.random.fold_in(key_of[14], 71), 0)
    query_key_value = draw_query_key_value(jax.random.fold_in(key_of[14], 71), 0)
    output_weight = gaussian(key_of[3], (D, D), D ** -0.5, 0.21875, ((0, 8),))
    up_weight = gaussian(key_of[4], (D, FF), D ** -0.5, 0.21875, ((0, 8),))
    down_weight = gaussian(key_of[5], (FF, D), FF ** -0.5, 0.109375, ((0, 8),))
    attention_gain = jnp.clip(1.0 + 0.15 * jax.random.normal(key_of[6], (D,), jnp.float32), 0.25, 1.75)
    feedforward_gain = jnp.clip(1.0 + 0.15 * jax.random.normal(key_of[7], (D,), jnp.float32), 0.25, 1.75)
    encoded = gaussian(key_of[8], (NODES, D), 1.0, 6.0, ((0, 32),))
    send_rows = place_ends(jax.random.randint(key_of[9], (DEVICES, DEVICES, CAP), 0, NODES_DEV), jax.random.fold_in(key_of[9], 1), 0, NODES_DEV - 1).astype(jnp.int32)
    send_count = draw_send_count(jax.random.fold_in(key_of[14], 71), 0)
    arrival_nodes = draw_arrival_nodes(jax.random.fold_in(key_of[14], 71), 0)
    sage_weight = gaussian(key_of[12], (2, D, H), D ** -0.5, 0.21875, ((1, 8),))
    node_gain = jnp.clip(1.0 + 0.15 * jax.random.normal(key_of[13], (H,), jnp.float32), 0.25, 1.75)
    return dict(hidden_states=hidden_states, title_tokens=title_tokens, query_key_value=query_key_value, output_weight=output_weight, up_weight=up_weight, down_weight=down_weight, attention_gain=attention_gain, feedforward_gain=feedforward_gain, encoded=encoded, send_rows=send_rows, send_count=send_count, arrival_nodes=arrival_nodes, sage_weight=sage_weight, node_gain=node_gain)


LN_EPSILON = 1e-12

def layer_norm(values, gain):
    center = values - lax.optimization_barrier(jnp.mean(values, axis=-1, keepdims=True))
    spread = lax.optimization_barrier(jnp.mean(center * center, axis=-1, keepdims=True))
    return center * lax.rsqrt(spread + LN_EPSILON) * gain

def encode_titles(states, tokens, query_key_value, output_weight, up_weight, down_weight, attention_gain, feedforward_gain):
    titles = states.shape[0]
    flat = states.reshape(titles * SEQ, D)
    live = tokens != 0
    projected = jnp.dot(flat, query_key_value, preferred_element_type=jnp.float32).astype(jnp.bfloat16)
    projected = lax.optimization_barrier(projected)
    projected = projected.reshape(titles, SEQ, 3, HEADS, HEAD_DIM).astype(jnp.float32)
    query_states = projected[:, :, 0]
    key_states = projected[:, :, 1]
    value_states = projected[:, :, 2]
    scores = jnp.einsum('tihd,tjhd->thij', query_states, key_states) * (1.0 / math.sqrt(HEAD_DIM))
    scores = jnp.where(live[:, None, None, :], scores, -jnp.inf)
    highest = lax.optimization_barrier(jnp.max(scores, axis=-1, keepdims=True))
    weights = jnp.exp(scores - highest)
    probs = (weights / lax.optimization_barrier(jnp.sum(weights, axis=-1, keepdims=True))).astype(jnp.bfloat16)
    probs = lax.optimization_barrier(probs)
    context = jnp.einsum('thij,tjhd->tihd', probs.astype(jnp.float32), value_states)
    context = context.astype(jnp.bfloat16).reshape(titles * SEQ, D)
    mixed = jnp.dot(context, output_weight, preferred_element_type=jnp.float32)
    attended = layer_norm(flat.astype(jnp.float32) + mixed, attention_gain).astype(jnp.bfloat16)
    attended = lax.optimization_barrier(attended)
    inner = jax.nn.gelu(jnp.dot(attended, up_weight, preferred_element_type=jnp.float32), approximate=False)
    inner = inner.astype(jnp.bfloat16)
    lowered = jnp.dot(inner, down_weight, preferred_element_type=jnp.float32)
    token_out = layer_norm(attended.astype(jnp.float32) + lowered, feedforward_gain).reshape(titles, SEQ, D)
    live_weight = live.astype(jnp.float32)
    pooled = lax.optimization_barrier(jnp.sum(token_out * live_weight[:, :, None], axis=1)) / lax.optimization_barrier(jnp.sum(live_weight, axis=1, keepdims=True))
    return pooled.astype(jnp.bfloat16)

def reference(hidden_states, title_tokens, query_key_value, output_weight, up_weight, down_weight, attention_gain, feedforward_gain, encoded, send_rows, send_count, arrival_nodes, sage_weight, node_gain):

    def one_device(element):
        return encode_titles(element[0], element[1], query_key_value, output_weight, up_weight, down_weight, attention_gain, feedforward_gain)
    pooled = lax.map(one_device, (hidden_states.reshape(DEVICES, TITLES_DEV, SEQ, D), title_tokens.reshape(DEVICES, TITLES_DEV, SEQ)))
    title_vectors = pooled.reshape(TITLES, D)
    sources = jnp.arange(DEVICES, dtype=jnp.int32)
    slots = jnp.arange(CAP, dtype=jnp.int32)

    def one_receiver(element):
        rows_from, counts_from, targets = element
        index = (sources[:, None] * NODES_DEV + rows_from).reshape(-1).astype(jnp.int32)
        rows = jnp.take(encoded, index, axis=0).astype(jnp.float32)
        valid = (slots[None, :] < counts_from[:, None]).reshape(-1).astype(jnp.float32)
        labels = targets.reshape(-1).astype(jnp.int32)
        sums = jax.ops.segment_sum(rows * valid[:, None], labels, num_segments=NODES_DEV)
        degree = jax.ops.segment_sum(valid, labels, num_segments=NODES_DEV)
        return (sums / jnp.maximum(degree, 1.0)[:, None]).astype(jnp.bfloat16)
    neighbour_mean = lax.map(one_receiver, (jnp.transpose(send_rows, (1, 0, 2)), jnp.transpose(send_count), arrival_nodes))
    neighbour_mean = neighbour_mean.reshape(NODES, D)
    own_rows = encoded.reshape(DEVICES, NODES_DEV, D)
    self_rows = jnp.concatenate([pooled, own_rows[:, TITLES_DEV:]], axis=1).reshape(NODES, D)
    combined = jnp.dot(self_rows, sage_weight[0], preferred_element_type=jnp.float32)
    combined = combined + jnp.dot(neighbour_mean, sage_weight[1], preferred_element_type=jnp.float32)
    node_output = layer_norm(combined, node_gain).astype(jnp.bfloat16)
    return (title_vectors, node_output)
```

```python
import functools
import math

import jax
import jax.numpy as jnp
from jax import lax
from jax.experimental import pallas as pl
from jax.experimental.pallas import tpu as pltpu
from jax.sharding import PartitionSpec as P


MESH = pl.DeviceIdType.MESH

HEAD_DIM = 64
PAIR = 2 * HEAD_DIM
LN_EPSILON = 1e-12
CHUNK = 256


def norm(values, gain):
    center = values - jnp.mean(values, axis=-1, keepdims=True)
    spread = jnp.mean(center * center, axis=-1, keepdims=True)
    return center * lax.rsqrt(spread + LN_EPSILON) * gain


def lengths(tokens, bias, lens):
    live = tokens[...] != 0
    bias[...] = jnp.where(live, 0.0, -1e30)
    count = jnp.sum(live.astype(jnp.float32), axis=1, keepdims=True)
    lens[...] = jnp.broadcast_to(count, lens.shape)


def project(states, weight, out, lo, hi, cols):
    @pl.loop(lo, hi)
    def _(j):
        c = pl.ds(pl.multiple_of(j * cols, cols), cols)
        out[:, c] = jnp.dot(states[...], weight[:, c], preferred_element_type=jnp.float32).astype(jnp.bfloat16)


def attend(qkv, bias, context, seq, lo, hi):
    width = context.shape[1]
    pairs = width // PAIR
    lane = lax.broadcasted_iota(jnp.int32, (1, PAIR), 1) < HEAD_DIM
    scale = 1.0 / math.sqrt(HEAD_DIM)
    first = jnp.where(lane, scale, 0.0).astype(jnp.bfloat16)
    second = jnp.where(lane, 0.0, scale).astype(jnp.bfloat16)
    ones = jnp.ones((seq, PAIR), jnp.bfloat16)
    side = jnp.broadcast_to(lane, (seq, PAIR))

    @pl.loop(lo, hi)
    def _(t):
        r = pl.ds(pl.multiple_of(t * seq, seq), seq)
        keys = bias[pl.ds(t, 1), :]
        for p in range(pairs):
            q = qkv[r, p * PAIR:(p + 1) * PAIR]
            k = qkv[r, width + p * PAIR:width + (p + 1) * PAIR]
            v = qkv[r, 2 * width + p * PAIR:2 * width + (p + 1) * PAIR]
            both = jnp.concatenate([q * first, q * second], axis=0)
            s = lax.dot_general(both, k, (((1,), (1,)), ((), ())), preferred_element_type=jnp.float32) + keys
            w = jnp.exp(s - jnp.max(s, axis=1, keepdims=True)).astype(jnp.bfloat16)
            o = jnp.dot(w, jnp.concatenate([v, ones], axis=1), preferred_element_type=jnp.float32)
            num = jnp.where(side, o[:seq, :PAIR], o[seq:, :PAIR])
            den = jnp.where(side, o[:seq, PAIR:], o[seq:, PAIR:])
            context[r, p * PAIR:(p + 1) * PAIR] = (num / den).astype(jnp.bfloat16)


def mix(context, weight, states, gain, attended, lo, hi, rows):
    @pl.loop(lo, hi)
    def _(i):
        r = pl.ds(pl.multiple_of(i * rows, rows), rows)
        mixed = jnp.dot(context[r, :], weight[...], preferred_element_type=jnp.float32)
        attended[r, :] = norm(states[r, :].astype(jnp.float32) + mixed, gain[...]).astype(jnp.bfloat16)


def widen(attended, weight, inner, lo, hi, cols):
    @pl.loop(lo, hi)
    def _(j):
        c = pl.ds(pl.multiple_of(j * cols, cols), cols)
        x = jnp.dot(attended[...], weight[:, c], preferred_element_type=jnp.float32)
        half = 0.5 * x
        inner[:, c] = (half + half * lax.erf(x * (1.0 / math.sqrt(2.0)))).astype(jnp.bfloat16)


def narrow(inner, weight, attended, gain, lens, pooled, seq, lo, hi, titles):
    rows = titles * seq
    place = lax.broadcasted_iota(jnp.int32, (seq, lens.shape[1]), 0).astype(jnp.float32)

    @pl.loop(lo, hi)
    def _(i):
        r = pl.ds(pl.multiple_of(i * rows, rows), rows)
        low = jnp.dot(inner[r, :], weight[...], preferred_element_type=jnp.float32)
        token = norm(attended[r, :].astype(jnp.float32) + low, gain[...])
        for k in range(titles):
            t = pl.ds(i * titles + k, 1)
            n = lens[t, :]
            part = jnp.where(place < n, token[k * seq:(k + 1) * seq], 0.0)
            pooled[t, :] = jnp.sum(part, axis=0, keepdims=True) / n


WORK = (
    ("project", 0, 0.7),
    ("attend", 0, 1.5),
    ("mix", 1, 1.5),
    ("widen", 2, 1.0),
    ("narrow", 3, 2.4),
)
RATE = 85e3
SLOW = 1.4


def plan(shard_bytes, outer, inner, steps, group):
    events = []
    start = 0.0
    for which, size in enumerate(shard_bytes):
        hop = size * (2 / 3) / RATE * SLOW
        events.append((max(0.0, start - 6.0), 0, ("own", which)))
        for k in range(outer):
            here = start + k * (hop + 1.7)
            if k:
                events.append((here, 1, ("z", which, k)))
            for over in range(inner):
                there = here if over == 0 else max(here, start + k * hop) + over * (hop + 1.7)
                if over:
                    events.append((there, 2, ("y", which, k, over)))
                if k or over:
                    events.append((there + 0.5 * hop + 1.7, 3, ("x", which, k, over)))
                    events.append((there + 0.5 * hop + 2.6, 4, ("c", which, k, over)))
        start += outer * hop * max(1, inner - 1)
    events.sort(key=lambda e: (e[0], e[1]))
    work = []
    for (name, which, cost), count, many in zip(WORK, steps, group):
        work += [((name, first, min(first + many, count)), which, cost * min(many, count - first)) for first in range(0, count, many)]
    left = [outer * inner - 1] * len(shard_bytes)
    order, now, at = [], 0.0, 0
    ready = set()
    for when, _, event in events:
        while at < len(work) and left[work[at][1]] == 0 and now + 0.5 * work[at][2] <= when:
            if work[at][1] not in ready:
                ready.add(work[at][1])
                order.append(("own_done", work[at][1]))
            order.append(("work",) + work[at][0])
            now += work[at][2]
            at += 1
        order.append(event)
        now = max(now, when)
        if event[0] == "c":
            left[event[1]] -= 1
    for item, which, _ in work[at:]:
        if which not in ready:
            ready.add(which)
            order.append(("own_done", which))
        order.append(("work",) + item)
    for which in range(len(shard_bytes)):
        if which not in ready:
            order.append(("own_done", which))
    return order


def encoder_kernel(outer, inner, seq, order, *refs):
    states, tokens, attention_gain, feedforward_gain = refs[:4]
    shards = refs[4:9]
    pooled_out, full_sage = refs[9:11]
    full_project, full_output, full_up, full_down = refs[11:15]
    projected, context, attended, inside, bias, lens, pooled = refs[15:22]
    (own_sem, z_send, z_recv, z_down, y_send, y_recv, x_send, x_recv, c_send, c_recv) = refs[22:]
    fulls = (full_project, full_output, full_up, full_down, full_sage)
    arity = len(shards)
    me = lax.axis_index("fsdp")
    spot = lax.axis_index("dom")
    row, column = me // inner, lax.rem(me, inner)
    base = (spot // 4) * 4
    side = lax.rem(spot, 4) // 2
    core = lax.rem(spot, 2)
    pair_peer = base + (1 - side) * 2 + core
    core_peer = base + side * 2 + (1 - core)
    outer_peers = [lax.rem(row + step, outer) * inner + column for step in range(1, outer)]
    inner_peers = [row * inner + lax.rem(column + step, inner) for step in range(1, inner)]

    nearest = [sorted(range(outer), key=lambda o: (abs(o - r), o)) for r in range(outer)]
    rows = []
    for k in range(outer):
        value = nearest[0][k]
        for r in range(1, outer):
            value = jnp.where(row == r, nearest[r][k], value)
        rows.append(value)

    barrier = pltpu.get_barrier_semaphore()
    for peer in outer_peers + inner_peers:
        pl.semaphore_signal(barrier, inc=1, device_id=(peer, spot), device_id_type=MESH)
    for peer in (pair_peer, core_peer):
        pl.semaphore_signal(barrier, inc=1, device_id=(me, peer), device_id_type=MESH)
    pl.semaphore_wait(barrier, outer + inner)

    def part(ref, start, count):
        if len(ref.shape) == 3:
            return ref.at[:, pl.ds(start, count), :]
        return ref.at[pl.ds(start, count), :]

    def rows_of(which):
        return shards[which].shape[-2]

    def unit_of(which):
        return rows_of(which) // 6

    def first_of(which):
        return (3 * core + side) * unit_of(which)

    def block_start(which, origin, over):
        owner = origin * inner + lax.rem(column - over + inner, inner)
        return owner * rows_of(which)

    def held(which, origin, over, first, count):
        return part(fulls[which], pl.multiple_of(block_start(which, origin, over) + first, 8), count)

    def remote(source, target, send, recv, device):
        return pltpu.make_async_remote_copy(
            src_ref=source, dst_ref=target, send_sem=send, recv_sem=recv, device_id=device, device_id_type=MESH
        )

    def own_copy(which):
        return pltpu.make_async_copy(shards[which], held(which, row, 0, 0, rows_of(which)), own_sem.at[which])

    def source_of(which, k, over):
        count = 2 * unit_of(which)
        if k == 0 and over == 0:
            return part(shards[which], pl.multiple_of(first_of(which), 8), count)
        return held(which, rows[k], over, first_of(which), count)

    def z_copy(which, k, to, send):
        return remote(
            source_of(which, k, 0),
            held(which, rows[k], 0, first_of(which), 2 * unit_of(which)),
            send,
            z_recv.at[which, rows[k]],
            (to * inner + column, spot),
        )

    def y_copy(which, k, over, receive=False):
        return remote(
            source_of(which, k, 0) if not receive else held(which, rows[k], over, first_of(which), 2 * unit_of(which)),
            held(which, rows[k], over if receive else 0, first_of(which), 2 * unit_of(which)),
            y_send.at[which, rows[k], over - 1],
            y_recv.at[which, rows[k], over - 1],
            (inner_peers[over - 1], spot),
        )

    def x_copy(which, k, over, receive=False):
        unit = unit_of(which)
        edge = 1 - side if receive else side
        piece = held(which, rows[k], over, (3 * core + 2 * edge) * unit, unit)
        return remote(piece, piece, x_send.at[which, rows[k], over], x_recv.at[which, rows[k], over], (me, pair_peer))

    def c_copy(which, k, over, receive=False):
        unit = unit_of(which)
        half = 1 - core if receive else core
        piece = held(which, rows[k], over, 3 * half * unit, 3 * unit)
        return remote(piece, piece, c_send.at[which, rows[k], over], c_recv.at[which, rows[k], over], (me, core_peer))

    def onward(k):
        up = rows[k] < row
        more = jnp.where(up, row + 1 < outer, row > 0)
        return more, jnp.where(up, row + 1, row - 1)

    def own(which):
        @pl.when(row + 1 < outer)
        def _():
            z_copy(which, 0, row + 1, z_send.at[which, row]).start()

        @pl.when(row > 0)
        def _():
            z_copy(which, 0, row - 1, z_down.at[which]).start()

        for over in range(1, inner):
            y_copy(which, 0, over).start()
        own_copy(which).start()

    def z_stage(which, k):
        z_copy(which, k, row, z_send.at[which, rows[k]]).wait_recv()
        more, to = onward(k)

        @pl.when(more)
        def _():
            z_copy(which, k, to, z_send.at[which, rows[k]]).start()

        for over in range(1, inner):
            y_copy(which, k, over).start()
        x_copy(which, k, 0).start()

    def y_stage(which, k, over):
        y_copy(which, k, over, receive=True).wait_recv()
        x_copy(which, k, over).start()

    def x_stage(which, k, over):
        x_copy(which, k, over, receive=True).wait_recv()
        c_copy(which, k, over).start()

    def c_stage(which, k, over):
        c_copy(which, k, over, receive=True).wait_recv()

    work = {
        "project": lambda lo, hi: project(states, full_project, projected, lo, hi, CHUNK),
        "attend": lambda lo, hi: attend(projected, bias, context, seq, lo, hi),
        "mix": lambda lo, hi: mix(context, full_output, states, attention_gain, attended, lo, hi, CHUNK),
        "widen": lambda lo, hi: widen(attended, full_up, inside, lo, hi, CHUNK),
        "narrow": lambda lo, hi: narrow(
            inside, full_down, attended, feedforward_gain, lens, pooled, seq, lo, hi, CHUNK // seq
        ),
    }
    stages = {
        "own": own,
        "z": z_stage,
        "y": y_stage,
        "x": x_stage,
        "c": c_stage,
        "own_done": lambda which: own_copy(which).wait(),
        "work": lambda name, lo, hi: work[name](lo, hi),
    }
    lengths(tokens, bias, lens)
    for item in order:
        stages[item[0]](*item[1:])
    pooled_out[...] = pooled[...].astype(pooled_out.dtype)

    for which in range(arity):
        @pl.when(row + 1 < outer)
        def _():
            z_copy(which, 0, row + 1, z_send.at[which, row]).wait_send()

        @pl.when(row > 0)
        def _():
            z_copy(which, 0, row - 1, z_down.at[which]).wait_send()

        for k in range(outer):
            if k:
                more, to = onward(k)

                @pl.when(more)
                def _():
                    z_copy(which, k, to, z_send.at[which, rows[k]]).wait_send()

            for over in range(inner):
                if over:
                    y_copy(which, k, over).wait_send()
                if k or over:
                    x_copy(which, k, over).wait_send()
                    c_copy(which, k, over).wait_send()


def encode_titles(fsdp, hidden_states, title_tokens, attention_gain, feedforward_gain, *weights):
    outer = 4 if fsdp % 4 == 0 else 1
    inner = fsdp // outer
    arity = len(weights)
    titles, seq, width = hidden_states.shape
    tokens_all = titles * seq
    shapes = []
    for weight in weights:
        shape = list(weight.shape)
        shape[-2] *= fsdp
        shapes.append(tuple(shape))
    hidden_units = shapes[2][1]
    steps = (shapes[0][1] // CHUNK, titles, tokens_all // CHUNK, hidden_units // CHUNK, tokens_all // CHUNK)
    sizes = [weight.size * weight.dtype.itemsize for weight in weights]
    order = plan(sizes, outer, inner, steps, (3, 2, 2, 3, 1))
    dma = pltpu.SemaphoreType.DMA
    vmem = pl.BlockSpec(memory_space=pltpu.VMEM)
    bf16, f32 = jnp.bfloat16, jnp.float32
    return pl.pallas_call(
        functools.partial(encoder_kernel, outer, inner, seq, order),
        out_shape=(jax.ShapeDtypeStruct((titles, width), bf16), jax.ShapeDtypeStruct(shapes[4], bf16)),
        in_specs=[vmem] * (4 + arity),
        out_specs=(vmem, pl.BlockSpec(memory_space=pl.ANY)),
        scratch_shapes=[pltpu.VMEM(shape, bf16) for shape in shapes[:4]]
        + [
            pltpu.VMEM((tokens_all, 3 * width), bf16),
            pltpu.VMEM((tokens_all, width), bf16),
            pltpu.VMEM((tokens_all, width), bf16),
            pltpu.VMEM((tokens_all, hidden_units), bf16),
            pltpu.VMEM((titles, seq), f32),
            pltpu.VMEM((titles, width), f32),
            pltpu.VMEM((titles, width), f32),
            dma((arity,)),
            dma((arity, outer)),
            dma((arity, outer)),
            dma((arity,)),
        ]
        + [dma((arity, outer, max(1, inner - 1)))] * 2
        + [dma((arity, outer, inner))] * 4,
        compiler_params=pltpu.CompilerParams(
            collective_id=0, has_side_effects=True, vmem_limit_bytes=56 * 2**20
        ),
        cost_estimate=pl.CostEstimate(flops=60_000_000_000, bytes_accessed=sum(sizes) * fsdp, transcendentals=0),
        name="encoder",
    )(hidden_states.reshape(tokens_all, width), title_tokens, attention_gain[None], feedforward_gain[None], *weights)


def sage_kernel(arrived, targets, encoded, titles, weight, gain, out):
    slots, width = arrived.shape
    nodes = encoded.shape[0]
    carried = arrived[:, :1] < jnp.inf
    rows = jnp.where(carried, arrived[...], 0.0).astype(jnp.bfloat16)
    marks = jnp.where(carried, jnp.ones((slots, 128), jnp.float32), 0.0).astype(jnp.bfloat16)
    for first in range(0, nodes, CHUNK):
        spots = lax.broadcasted_iota(jnp.int32, (CHUNK, slots), 0) + first
        pick = jnp.where(spots == targets[...], 1.0, 0.0).astype(jnp.bfloat16)
        sums = jnp.dot(pick, rows, preferred_element_type=jnp.float32)
        degree = jnp.maximum(jnp.dot(pick, marks, preferred_element_type=jnp.float32), 1.0)
        mean = (sums / jnp.concatenate([degree] * (width // 128), axis=1)).astype(jnp.bfloat16)
        own = encoded[first:first + CHUNK, :]
        if first == 0:
            count = titles.shape[0]
            own = jnp.concatenate([titles[...], own[count:]], axis=0)
        total = jnp.dot(own, weight[0], preferred_element_type=jnp.float32)
        total += jnp.dot(mean, weight[1], preferred_element_type=jnp.float32)
        out[first:first + CHUNK, :] = norm(total, gain[...]).astype(out.dtype)


def sage(arrived, targets, encoded, titles, weight, gain):
    vmem = pl.BlockSpec(memory_space=pltpu.VMEM)
    return pl.pallas_call(
        sage_kernel,
        out_shape=jax.ShapeDtypeStruct((encoded.shape[0], weight.shape[2]), jnp.bfloat16),
        in_specs=[vmem] * 6,
        out_specs=vmem,
        compiler_params=pltpu.CompilerParams(vmem_limit_bytes=56 * 2**20),
        cost_estimate=pl.CostEstimate(flops=3_000_000_000, bytes_accessed=7_000_000, transcendentals=0),
        name="sage",
    )(arrived, targets, encoded, titles, weight, gain[None])


def on_device(
    fsdp,
    hidden_states,
    title_tokens,
    query_key_value,
    output_weight,
    up_weight,
    down_weight,
    attention_gain,
    feedforward_gain,
    encoded,
    send_rows,
    send_count,
    arrival_nodes,
    sage_weight,
    node_gain,
):
    nodes, width = encoded.shape
    peers, slots = send_rows.shape[1:]
    picks = jax.nn.one_hot(send_rows[0].reshape(-1), nodes, dtype=jnp.bfloat16)
    sent = jnp.dot(picks, encoded, preferred_element_type=jnp.float32).astype(jnp.bfloat16)
    valid = jnp.arange(slots, dtype=jnp.int32)[None, :] < send_count[0][:, None]
    sent = jnp.where(valid[:, :, None], sent.reshape(peers, slots, width), jnp.inf)
    arrived = lax.all_to_all(sent, ("fsdp", "dom"), split_axis=0, concat_axis=0, tiled=True)
    title_vectors, full_sage = encode_titles(
        fsdp,
        hidden_states,
        title_tokens,
        attention_gain,
        feedforward_gain,
        query_key_value,
        output_weight,
        up_weight,
        down_weight,
        sage_weight,
    )
    node_output = sage(
        arrived.reshape(peers * slots, width),
        arrival_nodes[0].reshape(1, -1),
        encoded,
        title_vectors,
        full_sage,
        node_gain,
    )
    return (title_vectors, node_output)


def solution(mesh):
    return jax.shard_map(
        functools.partial(on_device, mesh.shape["fsdp"]),
        mesh=mesh,
        in_specs=(
            P(("fsdp", "dom"), None, None),
            P(("fsdp", "dom"), None),
            P("fsdp", None),
            P("fsdp", None),
            P("fsdp", None),
            P("fsdp", None),
            P(),
            P(),
            P(("fsdp", "dom"), None),
            P(("fsdp", "dom"), None, None),
            P(("fsdp", "dom"), None),
            P(("fsdp", "dom"), None, None),
            P(None, "fsdp", None),
            P(),
        ),
        out_specs=(P(("fsdp", "dom"), None), P(("fsdp", "dom"), None)),
        check_vma=False,
    )
```

```python
import functools
import heapq
import math

import jax
import jax.numpy as jnp
from jax import lax
from jax.experimental import pallas as pl
from jax.experimental.pallas import tpu as pltpu
from jax.sharding import PartitionSpec as P

MESH = pl.DeviceIdType.MESH

HEADS = 12
HEAD_DIM = 64
PAIR = 2 * HEAD_DIM
LN_EPSILON = 1e-12
CHUNK = 256


def norm(values, gain):
    center = values - jnp.mean(values, axis=-1, keepdims=True)
    spread = jnp.mean(center * center, axis=-1, keepdims=True)
    return center * lax.rsqrt(spread + LN_EPSILON) * gain

def lengths(tokens, bias, lens):
    live = tokens[...] != 0
    bias[...] = jnp.where(live, 0.0, -1e30)
    count = jnp.sum(live.astype(jnp.float32), axis=1, keepdims=True)
    lens[...] = jnp.broadcast_to(count, lens.shape)

def project(states, weight, out, lo, hi, cols):
    @pl.loop(lo, hi)
    def _(j):
        c = pl.ds(pl.multiple_of(j * cols, cols), cols)
        out[:, c] = jnp.dot(states[...], weight[:, c], preferred_element_type=jnp.float32).astype(jnp.bfloat16)

def attend(qkv, bias, context, seq, lo, hi):
    width = context.shape[1]
    pairs = width // PAIR
    lane = lax.broadcasted_iota(jnp.int32, (1, PAIR), 1) < HEAD_DIM
    scale = 1.0 / math.sqrt(HEAD_DIM)
    first = jnp.where(lane, scale, 0.0).astype(jnp.bfloat16)
    second = jnp.where(lane, 0.0, scale).astype(jnp.bfloat16)
    ones = jnp.ones((seq, PAIR), jnp.bfloat16)
    side = jnp.broadcast_to(lane, (seq, PAIR))
    @pl.loop(lo, hi)
    def _(t):
        r = pl.ds(pl.multiple_of(t * seq, seq), seq)
        keys = bias[pl.ds(t, 1), :]
        for p in range(pairs):
            q = qkv[r, p * PAIR:(p + 1) * PAIR]
            k = qkv[r, width + p * PAIR:width + (p + 1) * PAIR]
            v = qkv[r, 2 * width + p * PAIR:2 * width + (p + 1) * PAIR]
            both = jnp.concatenate([q * first, q * second], axis=0)
            s = lax.dot_general(both, k, (((1,), (1,)), ((), ())), preferred_element_type=jnp.float32) + keys
            w = jnp.exp(s - jnp.max(s, axis=1, keepdims=True)).astype(jnp.bfloat16)
            o = jnp.dot(w, jnp.concatenate([v, ones], axis=1), preferred_element_type=jnp.float32)
            num = jnp.where(side, o[:seq, :PAIR], o[seq:, :PAIR])
            den = jnp.where(side, o[:seq, PAIR:], o[seq:, PAIR:])
            context[r, p * PAIR:(p + 1) * PAIR] = (num / den).astype(jnp.bfloat16)

def mix(context, weight, states, gain, attended, lo, hi, rows):
    @pl.loop(lo, hi)
    def _(i):
        r = pl.ds(pl.multiple_of(i * rows, rows), rows)
        mixed = jnp.dot(context[r, :], weight[...], preferred_element_type=jnp.float32)
        attended[r, :] = norm(states[r, :].astype(jnp.float32) + mixed, gain[...].reshape(1, -1)).astype(jnp.bfloat16)

def widen(attended, weight, inner, lo, hi, cols):
    @pl.loop(lo, hi)
    def _(j):
        c = pl.ds(pl.multiple_of(j * cols, cols), cols)
        x = jnp.dot(attended[...], weight[:, c], preferred_element_type=jnp.float32)
        half = 0.5 * x
        inner[:, c] = (half + half * lax.erf(x * (1.0 / math.sqrt(2.0)))).astype(jnp.bfloat16)

def narrow(inner, weight, attended, gain, lens, pooled, seq, lo, hi, titles):
    rows = titles * seq
    place = lax.broadcasted_iota(jnp.int32, (seq, lens.shape[1]), 0).astype(jnp.float32)
    @pl.loop(lo, hi)
    def _(i):
        r = pl.ds(pl.multiple_of(i * rows, rows), rows)
        low = jnp.dot(inner[r, :], weight[...], preferred_element_type=jnp.float32)
        token = norm(attended[r, :].astype(jnp.float32) + low, gain[...].reshape(1, -1))
        for k in range(titles):
            t = pl.ds(i * titles + k, 1)
            n = lens[t, :]
            part = jnp.where(place < n, token[k * seq:(k + 1) * seq], 0.0)
            pooled[t, :] = jnp.sum(part, axis=0, keepdims=True) / n

def fill(table, wanted, counts, picks, outbox, slots, first, many):
    nodes, width = table.shape
    places = lax.broadcasted_iota(jnp.int32, (slots, nodes), 1)
    for j in range(many):
        column = wanted[:, first + j:first + j + 1]
        picks[j * slots:(j + 1) * slots, :] = jnp.where(places == column, 1.0, 0.0).astype(jnp.bfloat16)
    rows = jnp.dot(picks[...], table[...], preferred_element_type=jnp.float32)
    slot = lax.broadcasted_iota(jnp.int32, (slots, width), 0)
    for j in range(many):
        valid = slot < counts[:, first + j:first + j + 1]
        piece = jnp.where(valid, rows[j * slots:(j + 1) * slots, :], jnp.inf)
        outbox[(first + j) * slots:(first + j + 1) * slots, :] = piece.astype(jnp.bfloat16)


def collect(inbox, targets, sums, degree, slots, first, many):
    nodes, width = sums.shape
    arrived = inbox[first * slots:(first + many) * slots, :]
    carried = arrived[:, :1] < jnp.inf
    rows = jnp.where(carried, arrived, 0.0).astype(jnp.bfloat16)
    marks = jnp.where(carried, jnp.ones((many * slots, 128), jnp.float32), 0.0).astype(jnp.bfloat16)
    spots = lax.broadcasted_iota(jnp.int32, (nodes, many * slots), 0)
    pick = jnp.where(spots == targets[:, first * slots:(first + many) * slots], 1.0, 0.0).astype(jnp.bfloat16)
    more = jnp.dot(pick, rows, preferred_element_type=jnp.float32)
    count = jnp.dot(pick, marks, preferred_element_type=jnp.float32)
    if first == 0:
        sums[...] = more
        degree[...] = count
    else:
        sums[...] += more
        degree[...] += count


def join(sums, degree, table, pooled, weight, gain, out, lo, hi, rows):
    width = sums.shape[1]
    titles = pooled.shape[0]
    for first in range(lo * rows, hi * rows, rows):
        here = slice(first, first + rows)
        share = jnp.maximum(degree[here, :], 1.0)
        mean = (sums[here, :] / jnp.concatenate([share] * (width // 128), axis=1)).astype(jnp.bfloat16)
        own = table[here, :]
        if first == 0:
            own = jnp.concatenate([pooled[...], own[titles:].astype(jnp.float32)], axis=0).astype(jnp.bfloat16)
        total = jnp.dot(own, weight[0], preferred_element_type=jnp.float32)
        total += jnp.dot(mean, weight[1], preferred_element_type=jnp.float32)
        out[here, :] = norm(total, gain[...].reshape(1, -1)).astype(out.dtype)


WORK = (
    ("fill", None, 2.0),
    ("project", 0, 0.7),
    ("attend", 0, 1.4),
    ("mix", 1, 1.5),
    ("widen", 2, 0.95),
    ("narrow", 3, 2.4),
    ("collect", None, 1.6),
    ("join", 4, 1.6),
)
RATE = 46e3
SHARE = 1.0
LEAD = 40.0
HOP = 1.7
GIVE = (4.0, 60.0)


def nearest_rows(outer):
    return [sorted(range(outer), key=lambda o: (abs(o - r), o)) for r in range(outer)]


def arrivals(sizes, outer, inner):
    near = nearest_rows(outer)
    rate = RATE * SHARE
    free = [dict.fromkeys(("up", "down", "y", "x", "c"), 0.0) for _ in range(outer)]
    queue, times, count, start = [], {}, 0, 0.0
    for which, size in enumerate(sizes):
        for row in range(outer):
            heapq.heappush(queue, (max(0.0, start - LEAD), count, row, ("own", which)))
            count += 1
        start += outer * size / 3 / rate

    def send(now, row, link, size, target, event):
        nonlocal count
        begin = max(now, free[row][link])
        free[row][link] = begin + size / (500e3 if link == "c" else rate)
        heapq.heappush(queue, (free[row][link] + (0.9 if link == "c" else HOP), count, target, event))
        count += 1

    def onwards(now, row, which, origin, piece):
        if origin <= row < outer - 1:
            send(now, row, "up", piece, row + 1, ("z", which, origin))
        if origin >= row > 0:
            send(now, row, "down", piece, row - 1, ("z", which, origin))
        for over in range(1, inner):
            send(now, row, "y", piece, row, ("y", which, origin, over))

    while queue:
        now, _, row, event = heapq.heappop(queue)
        kind, which = event[:2]
        piece = sizes[which] / 3
        if kind == "own":
            key = event
            onwards(now, row, which, row, piece)
        else:
            origin = event[2]
            over = event[3] if kind != "z" else 0
            key = (kind, which, near[row].index(origin)) + ((over,) if kind != "z" else ())
            if kind == "z":
                onwards(now, row, which, origin, piece)
            if kind in "zy":
                send(now, row, "x", piece / 2, row, ("x", which, origin, over))
            elif kind == "x":
                send(now, row, "c", sizes[which] / 2, row, ("c", which, origin, over))
        times.setdefault(key, []).append(now)
    return times


def plan(sizes, outer, inner, steps, group, peers):
    rank = {"own": 0, "z": 1, "y": 2, "x": 3, "c": 4}
    events = [(max(v), rank[k[0]], k) for k, v in arrivals(sizes, outer, inner).items()]
    first, last = GIVE
    events += [(first + (last - first) * j / peers, 5, ("give", j)) for j in range(peers - 1)]
    events.sort()
    work = []
    for (name, which, cost), count, many in zip(WORK, steps, group):
        for at in range(0, count, many):
            work.append(((name, at, min(at + many, count)), which, cost * (min(at + many, count) - at)))
    left = [outer * inner - 1] * len(sizes)
    given = peers - 1
    order, now, at = [], 0.0, 0
    ready = set()

    def emit():
        nonlocal at, now
        item, which, cost = work[at]
        if which is not None and which not in ready:
            ready.add(which)
            order.append(("own_done", which))
        order.append(("work",) + item)
        now += cost
        at += 1

    filled = -(-steps[0] // group[0])
    for when, _, event in events:
        while at < len(work):
            item, which, cost = work[at]
            if which is not None and left[which]:
                break
            if item[0] == "collect" and (given or now < last + 12.0):
                break
            if now + 0.5 * cost > when and not (event[0] == "give" and at < filled):
                break
            emit()
        order.append(event)
        now = max(now, when)
        if event[0] == "c":
            left[event[1]] -= 1
        given -= event[0] == "give"
    while at < len(work):
        emit()
    return order


FILL = 16
STRIDE = 12
GROUP = (1, 3, 2, 2, 3, 1, 1, 1)


def encoder_kernel(outer, inner, dom_size, seq, order, *refs):
    hidden, tokens, attention_gain, feedforward_gain, node_gain, encoded, wanted, counts, targets = refs[:9]
    shards = refs[9:14]
    pooled_out, node_out = refs[14:16]
    full_project, full_output, full_up, full_down, full_sage = refs[16:21]
    states, table, inside, context, attended, outbox, inbox, picks, sums, degree, bias, lens, pooled = refs[21:34]
    (own_sem, z_send, z_recv, z_down, y_send, y_recv, x_send, x_recv, c_send, c_recv, load_sem, give_send, give_recv) = refs[34:]
    projected = inside.at[:, pl.ds(0, full_project.shape[1])]
    dom = dom_size
    fsdp = outer * inner
    peers = fsdp * dom
    slots = outbox.shape[0] // peers
    fulls = (full_project, full_output, full_up, full_down, full_sage)
    arity = len(shards)
    me = lax.axis_index("fsdp")
    spot = lax.axis_index("dom")
    row, column = me // inner, lax.rem(me, inner)
    base = (spot // 4) * 4
    side = lax.rem(spot, 4) // 2
    core = lax.rem(spot, 2)
    pair_peer = base + (1 - side) * 2 + core
    core_peer = base + side * 2 + (1 - core)
    outer_peers = [lax.rem(row + step, outer) * inner + column for step in range(1, outer)]
    inner_peers = [row * inner + lax.rem(column + step, inner) for step in range(1, inner)]

    nearest = nearest_rows(outer)
    rows = []
    for k in range(outer):
        value = nearest[0][k]
        for r in range(1, outer):
            value = jnp.where(row == r, nearest[r][k], value)
        rows.append(value)

    load_states = pltpu.make_async_copy(hidden, states, load_sem.at[0])
    load_table = pltpu.make_async_copy(encoded, table, load_sem.at[1])
    load_table.start()
    load_states.start()

    def peer_at(j):
        j = 1 + (j * STRIDE) % (peers - 1)
        return lax.rem(me + j // dom, fsdp), lax.rem(spot + j % dom, dom)

    barrier = pltpu.get_barrier_semaphore()
    for j in range(peers - 1):
        pl.semaphore_signal(barrier, inc=1, device_id=peer_at(j), device_id_type=MESH)
    pl.semaphore_wait(barrier, peers - 1)

    def part(ref, start, count):
        if len(ref.shape) == 3:
            return ref.at[:, pl.ds(start, count), :]
        return ref.at[pl.ds(start, count), :]

    def rows_of(which):
        return shards[which].shape[-2]

    def unit_of(which):
        return rows_of(which) // 6

    def first_of(which):
        return (3 * core + side) * unit_of(which)

    def block_start(which, origin, over):
        owner = origin * inner + lax.rem(column - over + inner, inner)
        return owner * rows_of(which)

    def held(which, origin, over, first, count):
        return part(fulls[which], pl.multiple_of(block_start(which, origin, over) + first, 8), count)

    def remote(source, target, send, recv, device):
        return pltpu.make_async_remote_copy(
            src_ref=source, dst_ref=target, send_sem=send, recv_sem=recv, device_id=device, device_id_type=MESH
        )

    def own_copy(which):
        return pltpu.make_async_copy(shards[which], held(which, row, 0, 0, rows_of(which)), own_sem.at[which])

    def source_of(which, k, over):
        count = 2 * unit_of(which)
        if k == 0 and over == 0:
            return part(shards[which], pl.multiple_of(first_of(which), 8), count)
        return held(which, rows[k], over, first_of(which), count)

    def z_copy(which, k, to, send):
        return remote(
            source_of(which, k, 0),
            held(which, rows[k], 0, first_of(which), 2 * unit_of(which)),
            send,
            z_recv.at[which, rows[k]],
            (to * inner + column, spot),
        )

    def y_copy(which, k, over, receive=False):
        return remote(
            source_of(which, k, 0) if not receive else held(which, rows[k], over, first_of(which), 2 * unit_of(which)),
            held(which, rows[k], over if receive else 0, first_of(which), 2 * unit_of(which)),
            y_send.at[which, rows[k], over - 1],
            y_recv.at[which, rows[k], over - 1],
            (inner_peers[over - 1], spot),
        )

    def x_copy(which, k, over, receive=False):
        unit = unit_of(which)
        edge = 1 - side if receive else side
        piece = held(which, rows[k], over, (3 * core + 2 * edge) * unit, unit)
        return remote(piece, piece, x_send.at[which, rows[k], over], x_recv.at[which, rows[k], over], (me, pair_peer))

    def c_copy(which, k, over, receive=False):
        unit = unit_of(which)
        half = 1 - core if receive else core
        piece = held(which, rows[k], over, 3 * half * unit, 3 * unit)
        return remote(piece, piece, c_send.at[which, rows[k], over], c_recv.at[which, rows[k], over], (me, core_peer))

    def onward(k):
        up = rows[k] < row
        more = jnp.where(up, row + 1 < outer, row > 0)
        return more, jnp.where(up, row + 1, row - 1)

    def own(which):
        @pl.when(row + 1 < outer)
        def _():
            z_copy(which, 0, row + 1, z_send.at[which, row]).start()

        @pl.when(row > 0)
        def _():
            z_copy(which, 0, row - 1, z_down.at[which]).start()

        for over in range(1, inner):
            y_copy(which, 0, over).start()
        own_copy(which).start()

    def z_stage(which, k):
        z_copy(which, k, row, z_send.at[which, rows[k]]).wait_recv()
        more, to = onward(k)

        @pl.when(more)
        def _():
            z_copy(which, k, to, z_send.at[which, rows[k]]).start()

        for over in range(1, inner):
            y_copy(which, k, over).start()
        x_copy(which, k, 0).start()

    def y_stage(which, k, over):
        y_copy(which, k, over, receive=True).wait_recv()
        x_copy(which, k, over).start()

    def x_stage(which, k, over):
        x_copy(which, k, over, receive=True).wait_recv()
        c_copy(which, k, over).start()

    def c_stage(which, k, over):
        c_copy(which, k, over, receive=True).wait_recv()

    index = me * dom + spot

    def box(ref, which):
        return ref.at[pl.ds(pl.multiple_of(which * slots, 16), slots)]

    def give_copy(j):
        there = peer_at(j)
        return remote(
            box(outbox, there[0] * dom + there[1]), box(inbox, index), give_send.at[j], give_recv.at[index], there
        )

    def take(source):
        @pl.when(index != source)
        def _():
            spot_in = box(inbox, source)
            remote(spot_in, spot_in, give_send.at[0], give_recv.at[source], peer_at(0)).wait_recv()

    def keep():
        return pltpu.make_async_copy(box(outbox, index), box(inbox, index), load_sem.at[2])

    def do_fill(lo, hi):
        if lo == 0:
            load_table.wait()
        fill(table, wanted, counts, picks, outbox, slots, lo * FILL, FILL)
        if hi * FILL == peers:
            keep().start()

    def do_collect(lo, hi):
        if lo == 0:
            keep().wait()
        for source in range(lo * FILL, hi * FILL):
            take(source)
        collect(inbox, targets, sums, degree, slots, lo * FILL, FILL)

    def do_project(lo, hi):
        if lo == 0:
            load_states.wait()
        project(states, full_project, projected, lo, hi, CHUNK)

    def do_join(lo, hi):
        join(sums, degree, table, pooled, full_sage, node_gain, node_out, lo, hi, CHUNK)

    titles = tokens.shape[0]
    work = {
        "fill": do_fill,
        "collect": do_collect,
        "join": do_join,
        "project": do_project,
        "attend": lambda lo, hi: attend(projected, bias, context, seq, lo, hi),
        "mix": lambda lo, hi: mix(context, full_output, states, attention_gain, attended, lo, hi, CHUNK),
        "widen": lambda lo, hi: widen(attended, full_up, inside, lo, hi, CHUNK),
        "narrow": lambda lo, hi: narrow(
            inside, full_down, attended, feedforward_gain, lens, pooled, seq, lo, hi, CHUNK // seq
        ),
    }
    stages = {
        "own": own,
        "give": lambda j: give_copy(j).start(),
        "z": z_stage,
        "y": y_stage,
        "x": x_stage,
        "c": c_stage,
        "own_done": lambda which: own_copy(which).wait(),
        "work": lambda name, lo, hi: work[name](lo, hi),
    }
    lengths(tokens, bias, lens)
    for item in order:
        stages[item[0]](*item[1:])
    pooled_out[...] = pooled[...].astype(pooled_out.dtype)

    for j in range(peers - 1):
        give_copy(j).wait_send()

    for which in range(arity):
        @pl.when(row + 1 < outer)
        def _():
            z_copy(which, 0, row + 1, z_send.at[which, row]).wait_send()

        @pl.when(row > 0)
        def _():
            z_copy(which, 0, row - 1, z_down.at[which]).wait_send()

        for k in range(outer):
            if k:
                more, to = onward(k)

                @pl.when(more)
                def _():
                    z_copy(which, k, to, z_send.at[which, rows[k]]).wait_send()

            for over in range(inner):
                if over:
                    y_copy(which, k, over).wait_send()
                if k or over:
                    x_copy(which, k, over).wait_send()
                    c_copy(which, k, over).wait_send()


def graph_layer(
    fsdp,
    dom,
    hidden_states,
    title_tokens,
    attention_gain,
    feedforward_gain,
    node_gain,
    encoded,
    send_rows,
    send_count,
    arrival_nodes,
    *weights,
):
    outer = 4 if fsdp % 4 == 0 else 1
    inner = fsdp // outer
    arity = len(weights)
    titles, seq, width = hidden_states.shape
    nodes = encoded.shape[0]
    peers, slots = send_rows.shape
    tokens_all = titles * seq
    shapes = []
    for weight in weights:
        shape = list(weight.shape)
        shape[-2] *= fsdp
        shapes.append(tuple(shape))
    hidden_units = shapes[2][1]
    groups = peers // FILL
    steps = (
        groups,
        shapes[0][1] // CHUNK,
        titles,
        tokens_all // CHUNK,
        hidden_units // CHUNK,
        tokens_all // CHUNK,
        groups,
        nodes // CHUNK,
    )
    sizes = [weight.size * weight.dtype.itemsize for weight in weights]
    order = plan(sizes, outer, inner, steps, GROUP, peers)
    dma = pltpu.SemaphoreType.DMA
    vmem = pl.BlockSpec(memory_space=pltpu.VMEM)
    anywhere = pl.BlockSpec(memory_space=pl.ANY)
    bf16, f32 = jnp.bfloat16, jnp.float32
    return pl.pallas_call(
        functools.partial(encoder_kernel, outer, inner, dom, seq, order),
        out_shape=(
            jax.ShapeDtypeStruct((titles, width), bf16),
            jax.ShapeDtypeStruct((nodes, shapes[4][2]), bf16),
        ),
        in_specs=[anywhere] + [vmem] * 4 + [anywhere] + [vmem] * 3 + [anywhere] * arity,
        out_specs=(vmem, vmem),
        scratch_shapes=[pltpu.VMEM(shape, bf16) for shape in shapes]
        + [
            pltpu.VMEM((tokens_all, width), bf16),
            pltpu.VMEM((nodes, width), bf16),
            pltpu.VMEM((tokens_all, hidden_units), bf16),
            pltpu.VMEM((tokens_all, width), bf16),
            pltpu.VMEM((tokens_all, width), bf16),
            pltpu.VMEM((peers * slots, width), bf16),
            pltpu.VMEM((peers * slots, width), bf16),
            pltpu.VMEM((FILL * slots, nodes), bf16),
            pltpu.VMEM((nodes, width), f32),
            pltpu.VMEM((nodes, 128), f32),
            pltpu.VMEM((titles, seq), f32),
            pltpu.VMEM((titles, width), f32),
            pltpu.VMEM((titles, width), f32),
            dma((arity,)),
            dma((arity, outer)),
            dma((arity, outer)),
            dma((arity,)),
        ]
        + [dma((arity, outer, max(1, inner - 1)))] * 2
        + [dma((arity, outer, inner))] * 4
        + [dma((3,)), dma((peers,)), dma((peers,))],
        compiler_params=pltpu.CompilerParams(
            collective_id=0, has_side_effects=True, vmem_limit_bytes=62 * 2**20
        ),
        cost_estimate=pl.CostEstimate(flops=20_000_000_000, bytes_accessed=sum(sizes) * fsdp, transcendentals=0),
        name="graph_layer",
    )(
        hidden_states.reshape(tokens_all, width),
        title_tokens,
        attention_gain,
        feedforward_gain,
        node_gain,
        encoded,
        send_rows.T,
        send_count,
        arrival_nodes.reshape(1, -1),
        *weights,
    )


def on_device(
    fsdp,
    dom,
    hidden_states,
    title_tokens,
    query_key_value,
    output_weight,
    up_weight,
    down_weight,
    attention_gain,
    feedforward_gain,
    encoded,
    send_rows,
    send_count,
    arrival_nodes,
    sage_weight,
    node_gain,
):
    return graph_layer(
        fsdp,
        dom,
        hidden_states,
        title_tokens,
        attention_gain,
        feedforward_gain,
        node_gain,
        encoded,
        send_rows[0],
        send_count,
        arrival_nodes[0],
        query_key_value,
        output_weight,
        up_weight,
        down_weight,
        sage_weight,
    )


def solution(mesh):
    return jax.shard_map(
        functools.partial(on_device, mesh.shape["fsdp"], mesh.shape["dom"]),
        mesh=mesh,
        in_specs=(
            P(("fsdp", "dom"), None, None),
            P(("fsdp", "dom"), None),
            P("fsdp", None),
            P("fsdp", None),
            P("fsdp", None),
            P("fsdp", None),
            P(),
            P(),
            P(("fsdp", "dom"), None),
            P(("fsdp", "dom"), None, None),
            P(("fsdp", "dom"), None),
            P(("fsdp", "dom"), None, None),
            P(None, "fsdp", None),
            P(),
        ),
        out_specs=(P(("fsdp", "dom"), None), P(("fsdp", "dom"), None)),
        check_vma=False,
    )
```

```python
import functools
import heapq
import math

import jax
import jax.numpy as jnp
from jax import lax
from jax.experimental import pallas as pl
from jax.experimental.pallas import tpu as pltpu
from jax.sharding import PartitionSpec as P

MESH = pl.DeviceIdType.MESH

HEADS = 12
HEAD_DIM = 64
PAIR = 2 * HEAD_DIM
LN_EPSILON = 1e-12
CHUNK = 256


def norm(values, gain):
    center = values - jnp.mean(values, axis=-1, keepdims=True)
    spread = jnp.mean(center * center, axis=-1, keepdims=True)
    return center * lax.rsqrt(spread + LN_EPSILON) * gain

def lengths(tokens, bias, lens):
    live = tokens[...] != 0
    bias[...] = jnp.where(live, 0.0, -1e30)
    count = jnp.sum(live.astype(jnp.float32), axis=1, keepdims=True)
    lens[...] = jnp.broadcast_to(count, lens.shape)

def project(states, weight, out, lo, hi, cols):
    @pl.loop(lo, hi)
    def _(j):
        c = pl.ds(pl.multiple_of(j * cols, cols), cols)
        out[:, c] = jnp.dot(states[...], weight[:, c], preferred_element_type=jnp.float32).astype(jnp.bfloat16)

def attend(qkv, bias, context, seq, lo, hi):
    width = context.shape[1]
    pairs = width // PAIR
    lane = lax.broadcasted_iota(jnp.int32, (1, PAIR), 1) < HEAD_DIM
    scale = 1.0 / math.sqrt(HEAD_DIM)
    first = jnp.where(lane, scale, 0.0).astype(jnp.bfloat16)
    second = jnp.where(lane, 0.0, scale).astype(jnp.bfloat16)
    ones = jnp.ones((seq, PAIR), jnp.bfloat16)
    side = jnp.broadcast_to(lane, (seq, PAIR))
    @pl.loop(lo, hi)
    def _(t):
        r = pl.ds(pl.multiple_of(t * seq, seq), seq)
        keys = bias[pl.ds(t, 1), :]
        for p in range(pairs):
            q = qkv[r, p * PAIR:(p + 1) * PAIR]
            k = qkv[r, width + p * PAIR:width + (p + 1) * PAIR]
            v = qkv[r, 2 * width + p * PAIR:2 * width + (p + 1) * PAIR]
            both = jnp.concatenate([q * first, q * second], axis=0)
            s = lax.dot_general(both, k, (((1,), (1,)), ((), ())), preferred_element_type=jnp.float32) + keys
            w = jnp.exp(s - jnp.max(s, axis=1, keepdims=True)).astype(jnp.bfloat16)
            o = jnp.dot(w, jnp.concatenate([v, ones], axis=1), preferred_element_type=jnp.float32)
            num = jnp.where(side, o[:seq, :PAIR], o[seq:, :PAIR])
            den = jnp.where(side, o[:seq, PAIR:], o[seq:, PAIR:])
            context[r, p * PAIR:(p + 1) * PAIR] = (num / den).astype(jnp.bfloat16)

def mix(context, weight, states, gain, attended, lo, hi, rows):
    @pl.loop(lo, hi)
    def _(i):
        r = pl.ds(pl.multiple_of(i * rows, rows), rows)
        mixed = jnp.dot(context[r, :], weight[...], preferred_element_type=jnp.float32)
        attended[r, :] = norm(states[r, :].astype(jnp.float32) + mixed, gain[...].reshape(1, -1)).astype(jnp.bfloat16)

def widen(attended, weight, inner, lo, hi, cols):
    @pl.loop(lo, hi)
    def _(j):
        c = pl.ds(pl.multiple_of(j * cols, cols), cols)
        x = jnp.dot(attended[...], weight[:, c], preferred_element_type=jnp.float32)
        half = 0.5 * x
        inner[:, c] = (half + half * lax.erf(x * (1.0 / math.sqrt(2.0)))).astype(jnp.bfloat16)

def narrow(inner, weight, attended, gain, lens, pooled, seq, lo, hi, titles):
    rows = titles * seq
    place = lax.broadcasted_iota(jnp.int32, (seq, lens.shape[1]), 0).astype(jnp.float32)
    @pl.loop(lo, hi)
    def _(i):
        r = pl.ds(pl.multiple_of(i * rows, rows), rows)
        low = jnp.dot(inner[r, :], weight[...], preferred_element_type=jnp.float32)
        token = norm(attended[r, :].astype(jnp.float32) + low, gain[...].reshape(1, -1))
        for k in range(titles):
            t = pl.ds(i * titles + k, 1)
            n = lens[t, :]
            part = jnp.where(place < n, token[k * seq:(k + 1) * seq], 0.0)
            pooled[t, :] = jnp.sum(part, axis=0, keepdims=True) / n

def upright(rows, square, columns):
    peers, slots = rows.shape[1:]
    square[...] = jnp.zeros(square.shape, square.dtype)
    square[:peers, :slots] = rows[0].astype(square.dtype)
    columns[...] = square[...].T


def one_hot(columns, picks, slots, first, many):
    places = lax.broadcasted_iota(jnp.int32, (slots, picks.shape[1]), 1).astype(jnp.float32)
    for j in range(many):
        column = columns[:slots, first + j:first + j + 1]
        picks[j * slots:(j + 1) * slots, :] = jnp.where(places == column, 1.0, 0.0).astype(jnp.bfloat16)


def fill(table, wanted, counts, picks, outbox, slots, first, many):
    width = table.shape[1]
    one_hot(wanted, picks, slots, first, many)
    rows = jnp.dot(picks[...], table[...], preferred_element_type=jnp.float32)
    slot = lax.broadcasted_iota(jnp.int32, (slots, width), 0)
    for j in range(many):
        valid = slot < counts[:, first + j:first + j + 1]
        piece = jnp.where(valid, rows[j * slots:(j + 1) * slots, :], jnp.inf)
        outbox[(first + j) * slots:(first + j + 1) * slots, :] = piece.astype(jnp.bfloat16)


def mark(targets, picks, hits, slots, first, many):
    one_hot(targets, picks, slots, first, many)
    hits[:, first * slots:(first + many) * slots] = picks[...].T


def collect(inbox, hits, sums, degree, slots, first, many):
    arrived = inbox[first * slots:(first + many) * slots, :]
    carried = arrived[:, :1] < jnp.inf
    rows = jnp.where(carried, arrived, 0.0).astype(jnp.bfloat16)
    marks = jnp.where(carried, jnp.ones((many * slots, 128), jnp.float32), 0.0).astype(jnp.bfloat16)
    pick = hits[:, first * slots:(first + many) * slots]
    more = jnp.dot(pick, rows, preferred_element_type=jnp.float32)
    count = jnp.dot(pick, marks, preferred_element_type=jnp.float32)
    if first == 0:
        sums[...] = more
        degree[...] = count
    else:
        sums[...] += more
        degree[...] += count


def join(sums, degree, table, pooled, weight, gain, out, lo, hi, rows):
    width = sums.shape[1]
    titles = pooled.shape[0]
    for first in range(lo * rows, hi * rows, rows):
        here = slice(first, first + rows)
        share = jnp.maximum(degree[here, :], 1.0)
        mean = (sums[here, :] / jnp.concatenate([share] * (width // 128), axis=1)).astype(jnp.bfloat16)
        own = table[here, :]
        if first == 0:
            own = jnp.concatenate([pooled[...], own[titles:].astype(jnp.float32)], axis=0).astype(jnp.bfloat16)
        total = jnp.dot(own, weight[0], preferred_element_type=jnp.float32)
        total += jnp.dot(mean, weight[1], preferred_element_type=jnp.float32)
        out[here, :] = norm(total, gain[...].reshape(1, -1)).astype(out.dtype)


WORK = (
    ("fill", None, 1.5, 1),
    ("mark", None, 1.5, 1),
    ("project", 0, 0.57, 2),
    ("attend", 0, 1.05, 1),
    ("mix", 1, 0.7, 1),
    ("widen", 2, 0.65, 2),
    ("narrow", 3, 1.7, 1),
    ("collect", None, 1.2, 1),
    ("join", 4, 1.5, 1),
)
NEEDS = {name: which for name, which, _, _ in WORK}
RATE = 46e3
SHARE = 1.0
LEAD = 8.0
HOP = 1.7
GIVE = (20.0, 80.0)

ORDER = (
    0, 4, 10, 6, 1, 2, 11, 5, 13, 55, 35, 12, 8, 17, 98, 30, 24, 42, 56, 14, 26, 31, 47, 61, 22, 67, 59, 33,
    3, 65, 57, 39, 43, 25, 36, 44, 15, 50, 46, 66, 68, 63, 85, 69, 23, 94, 9, 76, 16, 7, 51, 49, 52, 27, 28,
    71, 58, 78, 74, 72, 77, 79, 91, 82, 102, 90, 120, 45, 83, 73, 107, 87, 34, 92, 93, 64, 40, 96, 97, 100,
    54, 106, 95, 136, 41, 122, 84, 101, 116, 171, 111, 113, 105, 29, 149, 60, 19, 115, 80, 119, 38, 21, 104,
    170, 62, 134, 48, 110, 137, 108, 129, 144, 142, 162, 135, 128, 143, 18, 117, 118, 109, 151, 168, 114, 75,
    32, 20, 53, 70, 125, 88, 121, 124, 159, 126, 127, 132, 130, 112, 89, 131, 138, 140, 147, 150, 81, 148,
    157, 99, 155, 123, 153, 146, 166, 133, 152, 141, 103, 139, 156, 145, 86, 154, 37, 161, 164, 167, 163, 158,
    169, 165, 160, 172, 173, 174, 175,
)


def nearest_rows(outer):
    return [sorted(range(outer), key=lambda o: (abs(o - r), o)) for r in range(outer)]


def arrivals(sizes, outer, inner):
    near = nearest_rows(outer)
    rate = RATE * SHARE
    free = [dict.fromkeys(("up", "down", "y", "x", "c"), 0.0) for _ in range(outer)]
    queue, times, count, start = [], {}, 0, 0.0
    for which, size in enumerate(sizes):
        for row in range(outer):
            heapq.heappush(queue, (max(0.0, start - LEAD), count, row, ("own", which)))
            count += 1
        start += outer * size / 3 / rate

    def send(now, row, link, size, target, event):
        nonlocal count
        begin = max(now, free[row][link])
        free[row][link] = begin + size / (500e3 if link == "c" else rate)
        heapq.heappush(queue, (free[row][link] + (0.9 if link == "c" else HOP), count, target, event))
        count += 1

    def onwards(now, row, which, origin, piece):
        if origin <= row < outer - 1:
            send(now, row, "up", piece, row + 1, ("z", which, origin))
        if origin >= row > 0:
            send(now, row, "down", piece, row - 1, ("z", which, origin))
        for over in range(1, inner):
            send(now, row, "y", piece, row, ("y", which, origin, over))

    while queue:
        now, _, row, event = heapq.heappop(queue)
        kind, which = event[:2]
        piece = sizes[which] / 3
        if kind == "own":
            key = event
            onwards(now, row, which, row, piece)
        else:
            origin = event[2]
            over = event[3] if kind != "z" else 0
            key = (kind, which, near[row].index(origin)) + ((over,) if kind != "z" else ())
            if kind == "z":
                onwards(now, row, which, origin, piece)
            if kind in "zy":
                send(now, row, "x", piece / 2, row, ("x", which, origin, over))
            elif kind == "x":
                send(now, row, "c", sizes[which] / 2, row, ("c", which, origin, over))
        times.setdefault(key, []).append(now)
    return times


def plan(sizes, box, outer, inner, side, steps):
    peers = outer * inner * side * 2
    rank = {"own": 0, "z": 1, "y": 2, "x": 3, "c": 4}
    events = [(max(v), rank[k[0]], k) for k, v in arrivals(sizes, outer, inner).items()]
    first, last = GIVE
    events += [(first + (last - first) * j / peers, 5, ("give", j)) for j in range(peers - 1)]
    events.sort()
    work = []
    for (name, which, cost, many), count in zip(WORK, steps):
        for at in range(0, count, many):
            work.append((("work", name, at, min(at + many, count)), which, cost * (min(at + many, count) - at)))
    left = [outer * inner - 1] * len(sizes)
    given, now = peers - 1, 0.0
    order = []
    for when, _, event in events:
        while work:
            item, which, cost = work[0]
            early = item[1] in ("fill", "mark") and event[0] == "give"
            if which is not None and left[which] or item[1] == "collect" and given:
                break
            if now + 0.5 * cost > when and not early:
                break
            order.append(work.pop(0)[0])
            now += cost
        order.append(event)
        now = max(now, when)
        if event[0] == "c":
            left[event[1]] -= 1
        given -= event[0] == "give"
    order += [item for item, _, _ in work]
    if len(ORDER) == len(order):
        order = [order[i] for i in ORDER]
    ready, full = set(), []
    for event in order:
        need = NEEDS[event[1]] if event[0] == "work" else None
        if need is not None and need not in ready:
            ready.add(need)
            full.append(("own_done", need))
        full.append(event)
    return full


FILL = 16
STRIDE = 12


def encoder_kernel(outer, inner, dom_size, seq, order, *refs):
    hidden, tokens, attention_gain, feedforward_gain, node_gain, encoded, wanted, counts, targets = refs[:9]
    shards = refs[9:14]
    pooled_out, node_out = refs[14:16]
    full_project, full_output, full_up, full_down, full_sage = refs[16:21]
    states, table, inside, context, attended, outbox, inbox, picks, sums, degree, bias, lens, pooled, hits, square, wanted_at, target_at = refs[21:38]
    (own_sem, z_send, z_recv, z_down, y_send, y_recv, x_send, x_recv, c_send, c_recv, load_sem, give_send, give_recv) = refs[38:]
    projected = inside.at[:, pl.ds(0, full_project.shape[1])]
    dom = dom_size
    fsdp = outer * inner
    peers = fsdp * dom
    slots = outbox.shape[0] // peers
    fulls = (full_project, full_output, full_up, full_down, full_sage)
    arity = len(shards)
    me = lax.axis_index("fsdp")
    spot = lax.axis_index("dom")
    row, column = me // inner, lax.rem(me, inner)
    base = (spot // 4) * 4
    side = lax.rem(spot, 4) // 2
    core = lax.rem(spot, 2)
    pair_peer = base + (1 - side) * 2 + core
    core_peer = base + side * 2 + (1 - core)
    outer_peers = [lax.rem(row + step, outer) * inner + column for step in range(1, outer)]
    inner_peers = [row * inner + lax.rem(column + step, inner) for step in range(1, inner)]

    nearest = nearest_rows(outer)
    rows = []
    for k in range(outer):
        value = nearest[0][k]
        for r in range(1, outer):
            value = jnp.where(row == r, nearest[r][k], value)
        rows.append(value)

    load_states = pltpu.make_async_copy(hidden, states, load_sem.at[0])
    load_table = pltpu.make_async_copy(encoded, table, load_sem.at[1])
    load_table.start()
    load_states.start()

    def peer_at(j):
        j = 1 + (j * STRIDE) % (peers - 1)
        to_row = lax.rem(row + j // (peers // outer), outer)
        to_column = lax.rem(column + j // dom % inner, inner)
        to_side = lax.rem(spot // 2 + j % dom // 2, dom // 2)
        to_core = lax.rem(core + j % 2, 2)
        return to_row * inner + to_column, to_side * 2 + to_core

    barrier = pltpu.get_barrier_semaphore()
    for j in range(peers - 1):
        pl.semaphore_signal(barrier, inc=1, device_id=peer_at(j), device_id_type=MESH)
    pl.semaphore_wait(barrier, peers - 1)

    def part(ref, start, count):
        if len(ref.shape) == 3:
            return ref.at[:, pl.ds(start, count), :]
        return ref.at[pl.ds(start, count), :]

    def rows_of(which):
        return shards[which].shape[-2]

    def unit_of(which):
        return rows_of(which) // 6

    def first_of(which):
        return (3 * core + side) * unit_of(which)

    def block_start(which, origin, over):
        owner = origin * inner + lax.rem(column - over + inner, inner)
        return owner * rows_of(which)

    def held(which, origin, over, first, count):
        return part(fulls[which], pl.multiple_of(block_start(which, origin, over) + first, 8), count)

    def remote(source, target, send, recv, device):
        return pltpu.make_async_remote_copy(
            src_ref=source, dst_ref=target, send_sem=send, recv_sem=recv, device_id=device, device_id_type=MESH
        )

    def own_copy(which):
        return pltpu.make_async_copy(shards[which], held(which, row, 0, 0, rows_of(which)), own_sem.at[which])

    def source_of(which, k, over):
        count = 2 * unit_of(which)
        if k == 0 and over == 0:
            return part(shards[which], pl.multiple_of(first_of(which), 8), count)
        return held(which, rows[k], over, first_of(which), count)

    def z_copy(which, k, to, send):
        return remote(
            source_of(which, k, 0),
            held(which, rows[k], 0, first_of(which), 2 * unit_of(which)),
            send,
            z_recv.at[which, rows[k]],
            (to * inner + column, spot),
        )

    def y_copy(which, k, over, receive=False):
        return remote(
            source_of(which, k, 0) if not receive else held(which, rows[k], over, first_of(which), 2 * unit_of(which)),
            held(which, rows[k], over if receive else 0, first_of(which), 2 * unit_of(which)),
            y_send.at[which, rows[k], over - 1],
            y_recv.at[which, rows[k], over - 1],
            (inner_peers[over - 1], spot),
        )

    def x_copy(which, k, over, receive=False):
        unit = unit_of(which)
        edge = 1 - side if receive else side
        piece = held(which, rows[k], over, (3 * core + 2 * edge) * unit, unit)
        return remote(piece, piece, x_send.at[which, rows[k], over], x_recv.at[which, rows[k], over], (me, pair_peer))

    def c_copy(which, k, over, receive=False):
        unit = unit_of(which)
        half = 1 - core if receive else core
        piece = held(which, rows[k], over, 3 * half * unit, 3 * unit)
        return remote(piece, piece, c_send.at[which, rows[k], over], c_recv.at[which, rows[k], over], (me, core_peer))

    def onward(k):
        up = rows[k] < row
        more = jnp.where(up, row + 1 < outer, row > 0)
        return more, jnp.where(up, row + 1, row - 1)

    def own(which):
        @pl.when(row + 1 < outer)
        def _():
            z_copy(which, 0, row + 1, z_send.at[which, row]).start()

        @pl.when(row > 0)
        def _():
            z_copy(which, 0, row - 1, z_down.at[which]).start()

        for over in range(1, inner):
            y_copy(which, 0, over).start()
        own_copy(which).start()

    def z_stage(which, k):
        z_copy(which, k, row, z_send.at[which, rows[k]]).wait_recv()
        more, to = onward(k)

        @pl.when(more)
        def _():
            z_copy(which, k, to, z_send.at[which, rows[k]]).start()

        for over in range(1, inner):
            y_copy(which, k, over).start()
        x_copy(which, k, 0).start()

    def y_stage(which, k, over):
        y_copy(which, k, over, receive=True).wait_recv()
        x_copy(which, k, over).start()

    def x_stage(which, k, over):
        x_copy(which, k, over, receive=True).wait_recv()
        c_copy(which, k, over).start()

    def c_stage(which, k, over):
        c_copy(which, k, over, receive=True).wait_recv()

    index = me * dom + spot

    def box(ref, which):
        return ref.at[pl.ds(pl.multiple_of(which * slots, 16), slots)]

    def give_copy(j):
        there = peer_at(j)
        return remote(
            box(outbox, there[0] * dom + there[1]), box(inbox, index), give_send.at[j], give_recv.at[index], there
        )

    def take(source):
        @pl.when(index != source)
        def _():
            spot_in = box(inbox, source)
            remote(spot_in, spot_in, give_send.at[0], give_recv.at[source], peer_at(0)).wait_recv()

    def keep():
        return pltpu.make_async_copy(box(outbox, index), box(inbox, index), load_sem.at[2])

    def do_fill(lo, hi):
        if lo == 0:
            upright(wanted, square, wanted_at)
            load_table.wait()
        fill(table, wanted_at, counts, picks, outbox, slots, lo * FILL, FILL)
        if hi * FILL == peers:
            keep().start()

    def do_mark(lo, hi):
        if lo == 0:
            upright(targets, square, target_at)
        mark(target_at, picks, hits, slots, lo * FILL, FILL)

    def do_collect(lo, hi):
        if lo == 0:
            keep().wait()
        for source in range(lo * FILL, hi * FILL):
            take(source)
        collect(inbox, hits, sums, degree, slots, lo * FILL, FILL)

    def do_project(lo, hi):
        if lo == 0:
            load_states.wait()
        project(states, full_project, projected, lo, hi, CHUNK)

    def do_join(lo, hi):
        join(sums, degree, table, pooled, full_sage, node_gain, node_out, lo, hi, CHUNK)

    titles = tokens.shape[0]
    work = {
        "fill": do_fill,
        "mark": do_mark,
        "collect": do_collect,
        "join": do_join,
        "project": do_project,
        "attend": lambda lo, hi: attend(projected, bias, context, seq, lo, hi),
        "mix": lambda lo, hi: mix(context, full_output, states, attention_gain, attended, lo, hi, CHUNK),
        "widen": lambda lo, hi: widen(attended, full_up, inside, lo, hi, CHUNK),
        "narrow": lambda lo, hi: narrow(
            inside, full_down, attended, feedforward_gain, lens, pooled, seq, lo, hi, CHUNK // seq
        ),
    }
    stages = {
        "own": own,
        "give": lambda j: give_copy(j).start(),
        "z": z_stage,
        "y": y_stage,
        "x": x_stage,
        "c": c_stage,
        "own_done": lambda which: own_copy(which).wait(),
        "work": lambda name, lo, hi: work[name](lo, hi),
    }
    lengths(tokens, bias, lens)
    for item in order:
        stages[item[0]](*item[1:])
    pooled_out[...] = pooled[...].astype(pooled_out.dtype)

    for j in range(peers - 1):
        give_copy(j).wait_send()

    for which in range(arity):
        @pl.when(row + 1 < outer)
        def _():
            z_copy(which, 0, row + 1, z_send.at[which, row]).wait_send()

        @pl.when(row > 0)
        def _():
            z_copy(which, 0, row - 1, z_down.at[which]).wait_send()

        for k in range(outer):
            if k:
                more, to = onward(k)

                @pl.when(more)
                def _():
                    z_copy(which, k, to, z_send.at[which, rows[k]]).wait_send()

            for over in range(inner):
                if over:
                    y_copy(which, k, over).wait_send()
                if k or over:
                    x_copy(which, k, over).wait_send()
                    c_copy(which, k, over).wait_send()


def graph_layer(
    fsdp,
    dom,
    hidden_states,
    title_tokens,
    attention_gain,
    feedforward_gain,
    node_gain,
    encoded,
    send_rows,
    send_count,
    arrival_nodes,
    *weights,
):
    outer = 4 if fsdp % 4 == 0 else 1
    inner = fsdp // outer
    arity = len(weights)
    titles, seq, width = hidden_states.shape
    nodes = encoded.shape[0]
    peers, slots = send_rows.shape[1:]
    side = max(128, peers)
    tokens_all = titles * seq
    shapes = []
    for weight in weights:
        shape = list(weight.shape)
        shape[-2] *= fsdp
        shapes.append(tuple(shape))
    hidden_units = shapes[2][1]
    groups = peers // FILL
    steps = (
        groups,
        groups,
        shapes[0][1] // CHUNK,
        titles,
        tokens_all // CHUNK,
        hidden_units // CHUNK,
        tokens_all // CHUNK,
        groups,
        nodes // CHUNK,
    )
    sizes = [weight.size * weight.dtype.itemsize for weight in weights]
    order = plan(sizes, slots * width * 2, outer, inner, dom // 2, steps)
    dma = pltpu.SemaphoreType.DMA
    vmem = pl.BlockSpec(memory_space=pltpu.VMEM)
    anywhere = pl.BlockSpec(memory_space=pl.ANY)
    bf16, f32 = jnp.bfloat16, jnp.float32
    return pl.pallas_call(
        functools.partial(encoder_kernel, outer, inner, dom, seq, order),
        out_shape=(
            jax.ShapeDtypeStruct((titles, width), bf16),
            jax.ShapeDtypeStruct((nodes, shapes[4][2]), bf16),
        ),
        in_specs=[anywhere] + [vmem] * 4 + [anywhere] + [vmem] * 3 + [anywhere] * arity,
        out_specs=(vmem, vmem),
        scratch_shapes=[pltpu.VMEM(shape, bf16) for shape in shapes]
        + [
            pltpu.VMEM((tokens_all, width), bf16),
            pltpu.VMEM((nodes, width), bf16),
            pltpu.VMEM((tokens_all, hidden_units), bf16),
            pltpu.VMEM((tokens_all, width), bf16),
            pltpu.VMEM((tokens_all, width), bf16),
            pltpu.VMEM((peers * slots, width), bf16),
            pltpu.VMEM((peers * slots, width), bf16),
            pltpu.VMEM((FILL * slots, nodes), bf16),
            pltpu.VMEM((nodes, width), f32),
            pltpu.VMEM((nodes, 128), f32),
            pltpu.VMEM((titles, seq), f32),
            pltpu.VMEM((titles, width), f32),
            pltpu.VMEM((titles, width), f32),
            pltpu.VMEM((nodes, peers * slots), bf16),
            pltpu.VMEM((side, side), f32),
            pltpu.VMEM((side, side), f32),
            pltpu.VMEM((side, side), f32),
            dma((arity,)),
            dma((arity, outer)),
            dma((arity, outer)),
            dma((arity,)),
        ]
        + [dma((arity, outer, max(1, inner - 1)))] * 2
        + [dma((arity, outer, inner))] * 4
        + [dma((3,)), dma((peers,)), dma((peers,))],
        compiler_params=pltpu.CompilerParams(
            collective_id=0, has_side_effects=True, vmem_limit_bytes=62 * 2**20
        ),
        cost_estimate=pl.CostEstimate(flops=20_000_000_000, bytes_accessed=sum(sizes) * fsdp, transcendentals=0),
        name="graph_layer",
    )(
        hidden_states.reshape(tokens_all, width),
        title_tokens,
        attention_gain,
        feedforward_gain,
        node_gain,
        encoded,
        send_rows,
        send_count,
        arrival_nodes,
        *weights,
    )


def on_device(
    fsdp,
    dom,
    hidden_states,
    title_tokens,
    query_key_value,
    output_weight,
    up_weight,
    down_weight,
    attention_gain,
    feedforward_gain,
    encoded,
    send_rows,
    send_count,
    arrival_nodes,
    sage_weight,
    node_gain,
):
    return graph_layer(
        fsdp,
        dom,
        hidden_states,
        title_tokens,
        attention_gain,
        feedforward_gain,
        node_gain,
        encoded,
        send_rows,
        send_count,
        arrival_nodes,
        query_key_value,
        output_weight,
        up_weight,
        down_weight,
        sage_weight,
    )


def solution(mesh):
    return jax.shard_map(
        functools.partial(on_device, mesh.shape["fsdp"], mesh.shape["dom"]),
        mesh=mesh,
        in_specs=(
            P(("fsdp", "dom"), None, None),
            P(("fsdp", "dom"), None),
            P("fsdp", None),
            P("fsdp", None),
            P("fsdp", None),
            P("fsdp", None),
            P(),
            P(),
            P(("fsdp", "dom"), None),
            P(("fsdp", "dom"), None, None),
            P(("fsdp", "dom"), None),
            P(("fsdp", "dom"), None, None),
            P(None, "fsdp", None),
            P(),
        ),
        out_specs=(P(("fsdp", "dom"), None), P(("fsdp", "dom"), None)),
        check_vma=False,
    )
```

```python
import functools
import heapq
import math

import jax
import jax.numpy as jnp
from jax import lax
from jax.experimental import pallas as pl
from jax.experimental.pallas import tpu as pltpu
from jax.sharding import PartitionSpec as P

MESH = pl.DeviceIdType.MESH

HEADS = 12
HEAD_DIM = 64
PAIR = 2 * HEAD_DIM
LN_EPSILON = 1e-12
CHUNK = 256


def norm(values, gain):
    center = values - jnp.mean(values, axis=-1, keepdims=True)
    spread = jnp.mean(center * center, axis=-1, keepdims=True)
    return center * lax.rsqrt(spread + LN_EPSILON) * gain

def lengths(tokens, bias, lens):
    live = tokens[...] != 0
    bias[...] = jnp.where(live, 0.0, -1e30)
    count = jnp.sum(live.astype(jnp.float32), axis=1, keepdims=True)
    lens[...] = jnp.broadcast_to(count, lens.shape)

def project(states, weight, out, lo, hi, cols):
    @pl.loop(lo, hi)
    def _(j):
        c = pl.ds(pl.multiple_of(j * cols, cols), cols)
        out[:, c] = jnp.dot(states[...], weight[:, c], preferred_element_type=jnp.float32).astype(jnp.bfloat16)

def attend(qkv, bias, context, seq, lo, hi):
    width = context.shape[1]
    pairs = width // PAIR
    lane = lax.broadcasted_iota(jnp.int32, (1, PAIR), 1) < HEAD_DIM
    scale = 1.0 / math.sqrt(HEAD_DIM)
    first = jnp.where(lane, scale, 0.0).astype(jnp.bfloat16)
    second = jnp.where(lane, 0.0, scale).astype(jnp.bfloat16)
    ones = jnp.ones((seq, PAIR), jnp.bfloat16)
    side = jnp.broadcast_to(lane, (seq, PAIR))
    @pl.loop(lo, hi)
    def _(t):
        r = pl.ds(pl.multiple_of(t * seq, seq), seq)
        keys = bias[pl.ds(t, 1), :]
        for p in range(pairs):
            q = qkv[r, p * PAIR:(p + 1) * PAIR]
            k = qkv[r, width + p * PAIR:width + (p + 1) * PAIR]
            v = qkv[r, 2 * width + p * PAIR:2 * width + (p + 1) * PAIR]
            both = jnp.concatenate([q * first, q * second], axis=0)
            s = lax.dot_general(both, k, (((1,), (1,)), ((), ())), preferred_element_type=jnp.float32) + keys
            w = jnp.exp(s - jnp.max(s, axis=1, keepdims=True)).astype(jnp.bfloat16)
            o = jnp.dot(w, jnp.concatenate([v, ones], axis=1), preferred_element_type=jnp.float32)
            num = jnp.where(side, o[:seq, :PAIR], o[seq:, :PAIR])
            den = jnp.where(side, o[:seq, PAIR:], o[seq:, PAIR:])
            context[r, p * PAIR:(p + 1) * PAIR] = (num / den).astype(jnp.bfloat16)

def mix(context, weight, states, gain, attended, lo, hi, rows):
    @pl.loop(lo, hi)
    def _(i):
        r = pl.ds(pl.multiple_of(i * rows, rows), rows)
        mixed = jnp.dot(context[r, :], weight[...], preferred_element_type=jnp.float32)
        attended[r, :] = norm(states[r, :].astype(jnp.float32) + mixed, gain[...].reshape(1, -1)).astype(jnp.bfloat16)

def widen(attended, weight, inner, lo, hi, cols):
    @pl.loop(lo, hi)
    def _(j):
        c = pl.ds(pl.multiple_of(j * cols, cols), cols)
        x = jnp.dot(attended[...], weight[:, c], preferred_element_type=jnp.float32)
        half = 0.5 * x
        inner[:, c] = (half + half * lax.erf(x * (1.0 / math.sqrt(2.0)))).astype(jnp.bfloat16)

def narrow(inner, weight, attended, gain, lens, pooled, seq, lo, hi, titles):
    rows = titles * seq
    place = lax.broadcasted_iota(jnp.int32, (seq, lens.shape[1]), 0).astype(jnp.float32)
    @pl.loop(lo, hi)
    def _(i):
        r = pl.ds(pl.multiple_of(i * rows, rows), rows)
        low = jnp.dot(inner[r, :], weight[...], preferred_element_type=jnp.float32)
        token = norm(attended[r, :].astype(jnp.float32) + low, gain[...].reshape(1, -1))
        for k in range(titles):
            t = pl.ds(i * titles + k, 1)
            n = lens[t, :]
            part = jnp.where(place < n, token[k * seq:(k + 1) * seq], 0.0)
            pooled[t, :] = jnp.sum(part, axis=0, keepdims=True) / n

def upright(rows, square, columns):
    peers, slots = rows.shape[1:]
    square[...] = jnp.zeros(square.shape, square.dtype)
    square[:peers, :slots] = rows[0].astype(square.dtype)
    columns[...] = square[...].T


def one_hot(columns, picks, slots, first, many):
    places = lax.broadcasted_iota(jnp.int32, (slots, picks.shape[1]), 1).astype(jnp.float32)
    for j in range(many):
        column = columns[:slots, first + j:first + j + 1]
        picks[j * slots:(j + 1) * slots, :] = jnp.where(places == column, 1.0, 0.0).astype(jnp.bfloat16)


def fill(table, wanted, counts, picks, outbox, slots, first, many):
    width = table.shape[1]
    one_hot(wanted, picks, slots, first, many)
    rows = jnp.dot(picks[...], table[...], preferred_element_type=jnp.float32)
    slot = lax.broadcasted_iota(jnp.int32, (slots, width), 0)
    for j in range(many):
        valid = slot < counts[:, first + j:first + j + 1]
        piece = jnp.where(valid, rows[j * slots:(j + 1) * slots, :], jnp.inf)
        outbox[(first + j) * slots:(first + j + 1) * slots, :] = piece.astype(jnp.bfloat16)


def mark(targets, picks, hits, slots, first, many):
    one_hot(targets, picks, slots, first, many)
    hits[:, first * slots:(first + many) * slots] = picks[...].T


def collect(inbox, hits, sums, degree, slots, first, many):
    arrived = inbox[first * slots:(first + many) * slots, :]
    carried = arrived[:, :1] < jnp.inf
    rows = jnp.where(carried, arrived, 0.0).astype(jnp.bfloat16)
    marks = jnp.where(carried, jnp.ones((many * slots, 128), jnp.float32), 0.0).astype(jnp.bfloat16)
    pick = hits[:, first * slots:(first + many) * slots]
    more = jnp.dot(pick, rows, preferred_element_type=jnp.float32)
    count = jnp.dot(pick, marks, preferred_element_type=jnp.float32)
    if first == 0:
        sums[...] = more
        degree[...] = count
    else:
        sums[...] += more
        degree[...] += count


def join(sums, degree, table, pooled, weight, gain, out, lo, hi, rows):
    width = sums.shape[1]
    titles = pooled.shape[0]
    for first in range(lo * rows, hi * rows, rows):
        here = slice(first, first + rows)
        share = jnp.maximum(degree[here, :], 1.0)
        mean = (sums[here, :] / jnp.concatenate([share] * (width // 128), axis=1)).astype(jnp.bfloat16)
        own = table[here, :]
        if first == 0:
            own = jnp.concatenate([pooled[...], own[titles:].astype(jnp.float32)], axis=0).astype(jnp.bfloat16)
        total = jnp.dot(own, weight[0], preferred_element_type=jnp.float32)
        total += jnp.dot(mean, weight[1], preferred_element_type=jnp.float32)
        out[here, :] = norm(total, gain[...].reshape(1, -1)).astype(out.dtype)


WORK = (
    ("fill", None, 1.5, 1),
    ("mark", None, 1.5, 1),
    ("project", 0, 0.57, 2),
    ("attend", 0, 1.05, 1),
    ("mix", 1, 0.7, 1),
    ("widen", 2, 0.65, 2),
    ("narrow", 3, 1.7, 1),
    ("collect", None, 1.2, 1),
    ("join", 4, 1.5, 1),
)
NEEDS = {name: which for name, which, _, _ in WORK}
RATE = 46e3
SHARE = 1.0
LEAD = 8.0
HOP = 1.7
GIVE = (20.0, 80.0)

ORDER = (
    4, 0, 10, 1, 6, 2, 5, 13, 3, 12, 11, 8, 35, 109, 30, 16, 14, 46, 24, 31, 17, 168, 33, 59, 23, 65, 7, 56,
    25, 42, 9, 44, 18, 51, 26, 52, 58, 32, 47, 43, 67, 27, 63, 57, 22, 15, 68, 28, 155, 61, 50, 69, 71, 19,
    74, 34, 64, 94, 77, 79, 66, 49, 82, 91, 54, 87, 120, 21, 60, 92, 90, 96, 39, 36, 78, 38, 107, 29, 20, 72,
    100, 41, 75, 85, 48, 136, 137, 122, 102, 106, 104, 84, 171, 83, 111, 144, 113, 117, 53, 45, 70, 121, 88,
    97, 124, 95, 101, 76, 129, 142, 150, 143, 126, 80, 116, 115, 118, 146, 37, 134, 135, 139, 123, 149, 108,
    98, 89, 151, 62, 119, 55, 105, 127, 158, 81, 166, 131, 128, 157, 125, 138, 40, 99, 162, 114, 110, 103,
    140, 148, 130, 159, 141, 147, 112, 86, 132, 73, 153, 152, 160, 156, 133, 93, 161, 170, 163, 145, 164, 154,
    167, 165, 169, 172, 173, 174, 175,
)


def nearest_rows(outer):
    return [sorted(range(outer), key=lambda o: (abs(o - r), o)) for r in range(outer)]


def arrivals(sizes, outer, inner):
    near = nearest_rows(outer)
    rate = RATE * SHARE
    free = [dict.fromkeys(("up", "down", "y", "x", "c"), 0.0) for _ in range(outer)]
    queue, times, count, start = [], {}, 0, 0.0
    for which, size in enumerate(sizes):
        for row in range(outer):
            heapq.heappush(queue, (max(0.0, start - LEAD), count, row, ("own", which)))
            count += 1
        start += outer * size / 3 / rate

    def send(now, row, link, size, target, event):
        nonlocal count
        begin = max(now, free[row][link])
        free[row][link] = begin + size / (500e3 if link == "c" else rate)
        heapq.heappush(queue, (free[row][link] + (0.9 if link == "c" else HOP), count, target, event))
        count += 1

    def onwards(now, row, which, origin, piece):
        if origin <= row < outer - 1:
            send(now, row, "up", piece, row + 1, ("z", which, origin))
        if origin >= row > 0:
            send(now, row, "down", piece, row - 1, ("z", which, origin))
        for over in range(1, inner):
            send(now, row, "y", piece, row, ("y", which, origin, over))

    while queue:
        now, _, row, event = heapq.heappop(queue)
        kind, which = event[:2]
        piece = sizes[which] / 3
        if kind == "own":
            key = event
            onwards(now, row, which, row, piece)
        else:
            origin = event[2]
            over = event[3] if kind != "z" else 0
            key = (kind, which, near[row].index(origin)) + ((over,) if kind != "z" else ())
            if kind == "z":
                onwards(now, row, which, origin, piece)
            if kind in "zy":
                send(now, row, "x", piece / 2, row, ("x", which, origin, over))
            elif kind == "x":
                send(now, row, "c", sizes[which] / 2, row, ("c", which, origin, over))
        times.setdefault(key, []).append(now)
    return times


def plan(sizes, box, outer, inner, side, steps):
    peers = outer * inner * side * 2
    rank = {"own": 0, "z": 1, "y": 2, "x": 3, "c": 4}
    events = [(max(v), rank[k[0]], k) for k, v in arrivals(sizes, outer, inner).items()]
    first, last = GIVE
    events += [(first + (last - first) * j / peers, 5, ("give", j)) for j in range(peers - 1)]
    events.sort()
    work = []
    for (name, which, cost, many), count in zip(WORK, steps):
        for at in range(0, count, many):
            work.append((("work", name, at, min(at + many, count)), which, cost * (min(at + many, count) - at)))
    left = [outer * inner - 1] * len(sizes)
    given, now = peers - 1, 0.0
    order = []
    for when, _, event in events:
        while work:
            item, which, cost = work[0]
            early = item[1] in ("fill", "mark") and event[0] == "give"
            if which is not None and left[which] or item[1] == "collect" and given:
                break
            if now + 0.5 * cost > when and not early:
                break
            order.append(work.pop(0)[0])
            now += cost
        order.append(event)
        now = max(now, when)
        if event[0] == "c":
            left[event[1]] -= 1
        given -= event[0] == "give"
    order += [item for item, _, _ in work]
    if len(ORDER) == len(order):
        order = [order[i] for i in ORDER]
    ready, full = set(), []
    for event in order:
        need = NEEDS[event[1]] if event[0] == "work" else None
        if need is not None and need not in ready:
            ready.add(need)
            full.append(("own_done", need))
        full.append(event)
    return full


FILL = 16
STRIDE = 12


def encoder_kernel(outer, inner, dom_size, seq, order, *refs):
    hidden, tokens, attention_gain, feedforward_gain, node_gain, encoded, wanted, counts, targets = refs[:9]
    shards = refs[9:14]
    pooled_out, node_out = refs[14:16]
    full_project, full_output, full_up, full_down, full_sage = refs[16:21]
    states, table, inside, context, attended, outbox, inbox, picks, sums, degree, bias, lens, pooled, hits, square, wanted_at, target_at = refs[21:38]
    (own_sem, z_send, z_recv, z_down, y_send, y_recv, x_send, x_recv, c_send, c_recv, load_sem, give_send, give_recv) = refs[38:]
    projected = inside.at[:, pl.ds(0, full_project.shape[1])]
    dom = dom_size
    fsdp = outer * inner
    peers = fsdp * dom
    slots = outbox.shape[0] // peers
    fulls = (full_project, full_output, full_up, full_down, full_sage)
    arity = len(shards)
    me = lax.axis_index("fsdp")
    spot = lax.axis_index("dom")
    row, column = me // inner, lax.rem(me, inner)
    base = (spot // 4) * 4
    side = lax.rem(spot, 4) // 2
    core = lax.rem(spot, 2)
    pair_peer = base + (1 - side) * 2 + core
    core_peer = base + side * 2 + (1 - core)
    outer_peers = [lax.rem(row + step, outer) * inner + column for step in range(1, outer)]
    inner_peers = [row * inner + lax.rem(column + step, inner) for step in range(1, inner)]

    nearest = nearest_rows(outer)
    rows = []
    for k in range(outer):
        value = nearest[0][k]
        for r in range(1, outer):
            value = jnp.where(row == r, nearest[r][k], value)
        rows.append(value)

    load_states = pltpu.make_async_copy(hidden, states, load_sem.at[0])
    load_table = pltpu.make_async_copy(encoded, table, load_sem.at[1])
    load_table.start()
    load_states.start()

    def peer_at(j):
        j = 1 + (j * STRIDE) % (peers - 1)
        to_row = lax.rem(row + j // (peers // outer), outer)
        to_column = lax.rem(column + j // dom % inner, inner)
        to_side = lax.rem(spot // 2 + j % dom // 2, dom // 2)
        to_core = lax.rem(core + j % 2, 2)
        return to_row * inner + to_column, to_side * 2 + to_core

    barrier = pltpu.get_barrier_semaphore()
    for j in range(peers - 1):
        pl.semaphore_signal(barrier, inc=1, device_id=peer_at(j), device_id_type=MESH)
    pl.semaphore_wait(barrier, peers - 1)

    def part(ref, start, count):
        if len(ref.shape) == 3:
            return ref.at[:, pl.ds(start, count), :]
        return ref.at[pl.ds(start, count), :]

    def rows_of(which):
        return shards[which].shape[-2]

    def unit_of(which):
        return rows_of(which) // 6

    def first_of(which):
        return (3 * core + side) * unit_of(which)

    def block_start(which, origin, over):
        owner = origin * inner + lax.rem(column - over + inner, inner)
        return owner * rows_of(which)

    def held(which, origin, over, first, count):
        return part(fulls[which], pl.multiple_of(block_start(which, origin, over) + first, 8), count)

    def remote(source, target, send, recv, device):
        return pltpu.make_async_remote_copy(
            src_ref=source, dst_ref=target, send_sem=send, recv_sem=recv, device_id=device, device_id_type=MESH
        )

    def own_copy(which):
        return pltpu.make_async_copy(shards[which], held(which, row, 0, 0, rows_of(which)), own_sem.at[which])

    def source_of(which, k, over):
        count = 2 * unit_of(which)
        if k == 0 and over == 0:
            return part(shards[which], pl.multiple_of(first_of(which), 8), count)
        return held(which, rows[k], over, first_of(which), count)

    def z_copy(which, k, to, send):
        return remote(
            source_of(which, k, 0),
            held(which, rows[k], 0, first_of(which), 2 * unit_of(which)),
            send,
            z_recv.at[which, rows[k]],
            (to * inner + column, spot),
        )

    def y_copy(which, k, over, receive=False):
        return remote(
            source_of(which, k, 0) if not receive else held(which, rows[k], over, first_of(which), 2 * unit_of(which)),
            held(which, rows[k], over if receive else 0, first_of(which), 2 * unit_of(which)),
            y_send.at[which, rows[k], over - 1],
            y_recv.at[which, rows[k], over - 1],
            (inner_peers[over - 1], spot),
        )

    def x_copy(which, k, over, receive=False):
        unit = unit_of(which)
        edge = 1 - side if receive else side
        piece = held(which, rows[k], over, (3 * core + 2 * edge) * unit, unit)
        return remote(piece, piece, x_send.at[which, rows[k], over], x_recv.at[which, rows[k], over], (me, pair_peer))

    def c_copy(which, k, over, receive=False):
        unit = unit_of(which)
        half = 1 - core if receive else core
        piece = held(which, rows[k], over, 3 * half * unit, 3 * unit)
        return remote(piece, piece, c_send.at[which, rows[k], over], c_recv.at[which, rows[k], over], (me, core_peer))

    def onward(k):
        up = rows[k] < row
        more = jnp.where(up, row + 1 < outer, row > 0)
        return more, jnp.where(up, row + 1, row - 1)

    def own(which):
        @pl.when(row + 1 < outer)
        def _():
            z_copy(which, 0, row + 1, z_send.at[which, row]).start()

        @pl.when(row > 0)
        def _():
            z_copy(which, 0, row - 1, z_down.at[which]).start()

        for over in range(1, inner):
            y_copy(which, 0, over).start()
        own_copy(which).start()

    def z_stage(which, k):
        z_copy(which, k, row, z_send.at[which, rows[k]]).wait_recv()
        more, to = onward(k)

        @pl.when(more)
        def _():
            z_copy(which, k, to, z_send.at[which, rows[k]]).start()

        for over in range(1, inner):
            y_copy(which, k, over).start()
        x_copy(which, k, 0).start()

    def y_stage(which, k, over):
        y_copy(which, k, over, receive=True).wait_recv()
        x_copy(which, k, over).start()

    def x_stage(which, k, over):
        x_copy(which, k, over, receive=True).wait_recv()
        c_copy(which, k, over).start()

    def c_stage(which, k, over):
        c_copy(which, k, over, receive=True).wait_recv()

    index = me * dom + spot

    def box(ref, which):
        return ref.at[pl.ds(pl.multiple_of(which * slots, 16), slots)]

    def give_copy(j):
        there = peer_at(j)
        return remote(
            box(outbox, there[0] * dom + there[1]), box(inbox, index), give_send.at[j], give_recv.at[index], there
        )

    def take(source):
        @pl.when(index != source)
        def _():
            spot_in = box(inbox, source)
            remote(spot_in, spot_in, give_send.at[0], give_recv.at[source], peer_at(0)).wait_recv()

    def keep():
        return pltpu.make_async_copy(box(outbox, index), box(inbox, index), load_sem.at[2])

    def do_fill(lo, hi):
        if lo == 0:
            upright(wanted, square, wanted_at)
            load_table.wait()
        fill(table, wanted_at, counts, picks, outbox, slots, lo * FILL, FILL)
        if hi * FILL == peers:
            keep().start()

    def do_mark(lo, hi):
        if lo == 0:
            upright(targets, square, target_at)
        mark(target_at, picks, hits, slots, lo * FILL, FILL)

    def do_collect(lo, hi):
        if lo == 0:
            keep().wait()
        for source in range(lo * FILL, hi * FILL):
            take(source)
        collect(inbox, hits, sums, degree, slots, lo * FILL, FILL)

    def do_project(lo, hi):
        if lo == 0:
            load_states.wait()
        project(states, full_project, projected, lo, hi, CHUNK)

    def do_join(lo, hi):
        join(sums, degree, table, pooled, full_sage, node_gain, node_out, lo, hi, CHUNK)

    titles = tokens.shape[0]
    work = {
        "fill": do_fill,
        "mark": do_mark,
        "collect": do_collect,
        "join": do_join,
        "project": do_project,
        "attend": lambda lo, hi: attend(projected, bias, context, seq, lo, hi),
        "mix": lambda lo, hi: mix(context, full_output, states, attention_gain, attended, lo, hi, CHUNK),
        "widen": lambda lo, hi: widen(attended, full_up, inside, lo, hi, CHUNK),
        "narrow": lambda lo, hi: narrow(
            inside, full_down, attended, feedforward_gain, lens, pooled, seq, lo, hi, CHUNK // seq
        ),
    }
    stages = {
        "own": own,
        "give": lambda j: give_copy(j).start(),
        "z": z_stage,
        "y": y_stage,
        "x": x_stage,
        "c": c_stage,
        "own_done": lambda which: own_copy(which).wait(),
        "work": lambda name, lo, hi: work[name](lo, hi),
    }
    lengths(tokens, bias, lens)
    for item in order:
        stages[item[0]](*item[1:])
    pooled_out[...] = pooled[...].astype(pooled_out.dtype)

    for j in range(peers - 1):
        give_copy(j).wait_send()

    for which in range(arity):
        @pl.when(row + 1 < outer)
        def _():
            z_copy(which, 0, row + 1, z_send.at[which, row]).wait_send()

        @pl.when(row > 0)
        def _():
            z_copy(which, 0, row - 1, z_down.at[which]).wait_send()

        for k in range(outer):
            if k:
                more, to = onward(k)

                @pl.when(more)
                def _():
                    z_copy(which, k, to, z_send.at[which, rows[k]]).wait_send()

            for over in range(inner):
                if over:
                    y_copy(which, k, over).wait_send()
                if k or over:
                    x_copy(which, k, over).wait_send()
                    c_copy(which, k, over).wait_send()


def graph_layer(
    fsdp,
    dom,
    hidden_states,
    title_tokens,
    attention_gain,
    feedforward_gain,
    node_gain,
    encoded,
    send_rows,
    send_count,
    arrival_nodes,
    *weights,
):
    outer = 4 if fsdp % 4 == 0 else 1
    inner = fsdp // outer
    arity = len(weights)
    titles, seq, width = hidden_states.shape
    nodes = encoded.shape[0]
    peers, slots = send_rows.shape[1:]
    side = max(128, peers)
    tokens_all = titles * seq
    shapes = []
    for weight in weights:
        shape = list(weight.shape)
        shape[-2] *= fsdp
        shapes.append(tuple(shape))
    hidden_units = shapes[2][1]
    groups = peers // FILL
    steps = (
        groups,
        groups,
        shapes[0][1] // CHUNK,
        titles,
        tokens_all // CHUNK,
        hidden_units // CHUNK,
        tokens_all // CHUNK,
        groups,
        nodes // CHUNK,
    )
    sizes = [weight.size * weight.dtype.itemsize for weight in weights]
    order = plan(sizes, slots * width * 2, outer, inner, dom // 2, steps)
    dma = pltpu.SemaphoreType.DMA
    vmem = pl.BlockSpec(memory_space=pltpu.VMEM)
    anywhere = pl.BlockSpec(memory_space=pl.ANY)
    bf16, f32 = jnp.bfloat16, jnp.float32
    return pl.pallas_call(
        functools.partial(encoder_kernel, outer, inner, dom, seq, order),
        out_shape=(
            jax.ShapeDtypeStruct((titles, width), bf16),
            jax.ShapeDtypeStruct((nodes, shapes[4][2]), bf16),
        ),
        in_specs=[anywhere] + [vmem] * 4 + [anywhere] + [vmem] * 3 + [anywhere] * arity,
        out_specs=(vmem, vmem),
        scratch_shapes=[pltpu.VMEM(shape, bf16) for shape in shapes]
        + [
            pltpu.VMEM((tokens_all, width), bf16),
            pltpu.VMEM((nodes, width), bf16),
            pltpu.VMEM((tokens_all, hidden_units), bf16),
            pltpu.VMEM((tokens_all, width), bf16),
            pltpu.VMEM((tokens_all, width), bf16),
            pltpu.VMEM((peers * slots, width), bf16),
            pltpu.VMEM((peers * slots, width), bf16),
            pltpu.VMEM((FILL * slots, nodes), bf16),
            pltpu.VMEM((nodes, width), f32),
            pltpu.VMEM((nodes, 128), f32),
            pltpu.VMEM((titles, seq), f32),
            pltpu.VMEM((titles, width), f32),
            pltpu.VMEM((titles, width), f32),
            pltpu.VMEM((nodes, peers * slots), bf16),
            pltpu.VMEM((side, side), f32),
            pltpu.VMEM((side, side), f32),
            pltpu.VMEM((side, side), f32),
            dma((arity,)),
            dma((arity, outer)),
            dma((arity, outer)),
            dma((arity,)),
        ]
        + [dma((arity, outer, max(1, inner - 1)))] * 2
        + [dma((arity, outer, inner))] * 4
        + [dma((3,)), dma((peers,)), dma((peers,))],
        compiler_params=pltpu.CompilerParams(
            collective_id=0, has_side_effects=True, vmem_limit_bytes=62 * 2**20
        ),
        cost_estimate=pl.CostEstimate(flops=20_000_000_000, bytes_accessed=sum(sizes) * fsdp, transcendentals=0),
        name="graph_layer",
    )(
        hidden_states.reshape(tokens_all, width),
        title_tokens,
        attention_gain,
        feedforward_gain,
        node_gain,
        encoded,
        send_rows,
        send_count,
        arrival_nodes,
        *weights,
    )


def on_device(
    fsdp,
    dom,
    hidden_states,
    title_tokens,
    query_key_value,
    output_weight,
    up_weight,
    down_weight,
    attention_gain,
    feedforward_gain,
    encoded,
    send_rows,
    send_count,
    arrival_nodes,
    sage_weight,
    node_gain,
):
    return graph_layer(
        fsdp,
        dom,
        hidden_states,
        title_tokens,
        attention_gain,
        feedforward_gain,
        node_gain,
        encoded,
        send_rows,
        send_count,
        arrival_nodes,
        query_key_value,
        output_weight,
        up_weight,
        down_weight,
        sage_weight,
    )


def solution(mesh):
    return jax.shard_map(
        functools.partial(on_device, mesh.shape["fsdp"], mesh.shape["dom"]),
        mesh=mesh,
        in_specs=(
            P(("fsdp", "dom"), None, None),
            P(("fsdp", "dom"), None),
            P("fsdp", None),
            P("fsdp", None),
            P("fsdp", None),
            P("fsdp", None),
            P(),
            P(),
            P(("fsdp", "dom"), None),
            P(("fsdp", "dom"), None, None),
            P(("fsdp", "dom"), None),
            P(("fsdp", "dom"), None, None),
            P(None, "fsdp", None),
            P(),
        ),
        out_specs=(P(("fsdp", "dom"), None), P(("fsdp", "dom"), None)),
        check_vma=False,
    )
```
